128 devices in a mesh: op: 32 (over z_lo, x, y), sector: 4 (over z_hi, core).
Axes of the slice: x: 4, y: 4, z: 4 (z_hi: 2, z_lo: 2; z = z_hi * 2 + z_lo), core: 2. Of those that a mesh axis runs over, the one named last changes fastest.
Arguments:
- wavefunction: bfloat16 [8, 512, 512], P('sector'), may hold values from -10 to 10
- left_blocks: bfloat16 [128, 8, 512, 512], P('op', 'sector'), may hold values from -1 to 1
- right_blocks: bfloat16 [128, 8, 512, 512], P('op', 'sector'), may hold values from -1 to 1
- target_sector: int32 [128, 8], P('op', 'sector'), may hold values from 0 to 7, as said below
- preconditioner: float32 [8, 512, 512], P('sector', 'op'), may hold values from 1 to 10
Outputs:
- sigma_first: float32 [8, 512, 512], P('sector', 'op')
- sigma_second: float32 [8, 512, 512], P('sector', 'op')
The draws below stay inside these ranges and needn't reach their ends.
Inputs may be any that keep to these rules, and one draw needn't show every extreme that they name: `target_sector`: sector t belongs to index t // 2 of sector. Among the 4 x 2 pairs (k, s) that one device holds, at most 3 have targets belonging to one index of sector, and on every device some index of sector gets exactly 3.
All inputs are finite; a program needn't handle non-finite values.
Results may differ from the reference program's by a relative error of at most 0.0034.
Values may be sent and summed in bfloat16 or wider, within the bound.
No kernel may reach another device: no remote copies, remote signals or barrier semaphores. Data moves between devices by JAX's collectives and lax.ppermute only.
A program may use at most 64 MiB of HBM per device.

```python
import math
import jax
import jax.numpy as jnp
from jax import lax

BLOCK = 512
SEC_DEV = 2
TERM_DEV = 4
NSEC = 8
TERMS = 128


def device_owners(key, favourite):
    owner_count = NSEC // SEC_DEV
    task_count = TERM_DEV * SEC_DEV
    limit = (task_count + owner_count - 1) // owner_count + 1
    pick_key, hot_key, perm_key, order_key = jax.random.split(key, 4)
    random_hot = jax.random.randint(hot_key, (), 0, owner_count)
    use_fav = jax.random.randint(pick_key, (), 0, 2)
    hot_owner = jnp.where(use_fav == 1, favourite, random_hot)
    others = (hot_owner + 1 + jnp.arange((owner_count - 1) * limit) // limit) % owner_count
    others = jax.random.permutation(perm_key, others)
    owners = jnp.concatenate([jnp.full((limit,), hot_owner, jnp.int32), others[:task_count - limit].astype(jnp.int32)])
    return jax.random.permutation(order_key, owners)


def draw_target_sector(key, part):
    owner_count = NSEC // SEC_DEV
    op_count = TERMS // TERM_DEV
    device_count = op_count * owner_count
    fav_key, dev_key, low_key = jax.random.split(jax.random.fold_in(key, 7), 3)
    favourite = jax.random.randint(fav_key, (), 0, owner_count)
    keys = jax.random.split(dev_key, device_count)
    owners = jax.vmap(lambda single: device_owners(single, favourite))(keys)
    low = jax.random.randint(low_key, owners.shape, 0, SEC_DEV)
    targets = owners * SEC_DEV + low
    targets = targets.reshape(op_count, owner_count, TERM_DEV, SEC_DEV)
    targets = jnp.transpose(targets, (0, 2, 1, 3)).reshape(TERMS, NSEC)
    return targets.astype(jnp.int32)


def draw_wavefunction(key, part):
    own_key = jax.random.fold_in(key, 11)
    position = jnp.arange(BLOCK, dtype=jnp.float32) / (BLOCK - 1)
    values = jnp.clip(jax.random.normal(own_key, (NSEC, BLOCK, BLOCK), jnp.float32), -4.0, 4.0)
    scales = 2.5 ** position
    return (values * scales[None, :, None]).astype(jnp.bfloat16)


def operator_draw(key, spread, diagonal):
    shape = (TERMS, NSEC, BLOCK, BLOCK)
    values = jnp.clip(jax.random.normal(key, shape, jnp.float32), -3.0, 3.0)
    identity = jnp.eye(BLOCK, dtype=jnp.float32)
    return (values * spread + diagonal * identity[None, None]).astype(jnp.bfloat16)


def draw_left_blocks(key, part):
    own_key = jax.random.fold_in(key, 23)
    spread = 1.0 / (BLOCK * TERMS) ** 0.5
    return operator_draw(own_key, spread, 0.5 / TERMS ** 0.5)


def draw_right_blocks(key, part):
    own_key = jax.random.fold_in(key, 29)
    spread = 1.0 / BLOCK ** 0.5
    return operator_draw(own_key, spread, 0.5)


def levels(rng, dims, cuts, low, largest):
    factor_of, own = 1.0, jax.random.fold_in(rng, 6)
    for axis_at, blocks in cuts:
        steps = jnp.exp(jax.random.uniform(jax.random.fold_in(own, axis_at), (blocks,), jnp.float32, low / len(cuts), largest / len(cuts)))
        factor_of = factor_of * jnp.repeat(steps, dims[axis_at] // blocks).reshape([-1 if axis == axis_at else 1 for axis in range(len(dims))])
    return factor_of


def setup_inputs(seed: int = 0) -> dict:
    seeds = jax.random.split(jax.random.key(seed), 6)
    wavefunction = draw_wavefunction(jax.random.fold_in(seeds[5], 71), 0)
    left_blocks = draw_left_blocks(jax.random.fold_in(seeds[5], 71), 0)
    right_blocks = draw_right_blocks(jax.random.fold_in(seeds[5], 71), 0)
    target_sector = draw_target_sector(jax.random.fold_in(seeds[5], 71), 0)
    preconditioner = jnp.clip(jnp.exp(math.log(10.0) - 2.3025851 * jax.random.uniform(seeds[4], (NSEC, BLOCK, BLOCK), jnp.float32) ** levels(seeds[4], (NSEC, BLOCK, BLOCK), ((0, 4), (1, 32)), -0.2, 0.2)), 1.0, 10.0)
    return dict(wavefunction=wavefunction, left_blocks=left_blocks, right_blocks=right_blocks, target_sector=target_sector, preconditioner=preconditioner)


def apply_terms(left_blocks, right_blocks, target_sector, vector):
    term_count, sector_count = target_sector.shape
    block_width = vector.shape[1]

    def one_task(task_index, totals):
        term_index = task_index // sector_count
        sector_index = task_index % sector_count
        middle = jnp.dot(left_blocks[term_index, sector_index], vector[sector_index], preferred_element_type=jnp.float32).astype(jnp.bfloat16)
        contribution = lax.dot_general(middle, right_blocks[term_index, sector_index], (((1,), (1,)), ((), ())), preferred_element_type=jnp.float32)
        target = target_sector[term_index, sector_index]
        return totals.at[target].add(contribution)
    initial = jnp.zeros((sector_count, block_width, block_width), jnp.float32)
    return lax.fori_loop(0, term_count * sector_count, one_task, initial)

def reference(wavefunction, left_blocks, right_blocks, target_sector, preconditioner):
    sigma_first = apply_terms(left_blocks, right_blocks, target_sector, wavefunction)
    floats = wavefunction.astype(jnp.float32)
    norm_sq = jnp.sum(floats * floats)
    rayleigh = jnp.sum(floats * sigma_first) / norm_sq
    correction = (sigma_first - (rayleigh - 1.0) * floats) / preconditioner
    update = correction - jnp.sum(floats * correction) / norm_sq * floats
    new_vector = (update * jnp.sqrt(norm_sq) * lax.rsqrt(jnp.sum(update * update) + 1e-06)).astype(jnp.bfloat16)
    sigma_second = apply_terms(left_blocks, right_blocks, target_sector, new_vector)
    return (sigma_first, sigma_second)
```

```python
import functools

import jax
import jax.numpy as jnp
from jax import lax
from jax.experimental import pallas as pl
from jax.experimental.pallas import tpu as pltpu
from jax.sharding import Mesh
from jax.sharding import PartitionSpec as P

SECTOR = ("sector_0", "sector_1")
OP = ("op_0", "op_1", "op_2")
CHIPS = ("op_0", "op_1", "op_2", "sector_0")
EVERY = ("op_0", "op_1", "op_2", "sector_0", "sector_1")
CORE = "sector_1"
F32 = jnp.float32
BF16 = jnp.bfloat16
VMEM = pl.BlockSpec(memory_space=pltpu.VMEM)
SMEM = pl.BlockSpec(memory_space=pltpu.SMEM)
HBM = pl.BlockSpec(memory_space=pltpu.HBM)


def room(mebibytes):
    return pltpu.CompilerParams(vmem_limit_bytes=mebibytes * 2**20)


def exchange(pieces, axis):
    return lax.all_to_all(pieces, axis, split_axis=0, concat_axis=0, tiled=True)


def wanted(targets, core, local_sectors, task):
    return lax.rem(targets[task] // local_sectors, 2) == core[0]


def all_tasks(targets, core, local_sectors, vector, lefts, rights, totals, arrive):
    tasks, width, _ = lefts.shape
    totals[...] = jnp.zeros_like(totals)

    def one_task(task, carry):
        @pl.when(wanted(targets, core, local_sectors, task))
        def _():
            arrive(task)
            sector = lax.rem(task, local_sectors)
            source = vector[sector] if vector.shape[1] == width else vector[:, sector]
            source = source.reshape(width, width)
            middle = jnp.dot(lefts[task], source, preferred_element_type=F32).astype(BF16)
            target = targets[task]
            slot = target // (2 * local_sectors) * local_sectors + lax.rem(target, local_sectors)
            totals[slot] += lax.dot_general(
                middle, rights[task], (((1,), (1,)), ((), ())), preferred_element_type=F32
            )

        return carry

    lax.fori_loop(0, tasks, one_task, 0)


def loading_kernel(local_sectors, targets, core, vector, left, right, totals, lefts, rights, sems):

    def copies(task):
        return (
            pltpu.make_async_copy(left.at[task], lefts.at[task], sems.at[0, task]),
            pltpu.make_async_copy(right.at[task], rights.at[task], sems.at[1, task]),
        )

    def start(task, carry):
        @pl.when(wanted(targets, core, local_sectors, task))
        def _():
            for copy in copies(task):
                copy.start()

        return carry

    def arrive(task):
        for copy in copies(task):
            copy.wait()

    lax.fori_loop(0, left.shape[0], start, 0)
    all_tasks(targets, core, local_sectors, vector, lefts, rights, totals, arrive)


def resident_kernel(local_sectors, targets, core, vector, lefts, rights, totals):
    all_tasks(targets, core, local_sectors, vector, lefts, rights, totals, lambda task: None)


def apply_terms(targets, core, vector, left, right, loading):
    tasks, width, _ = left.shape
    slots = tasks // 2
    total = jax.ShapeDtypeStruct((slots, width, width), F32)
    cost = pl.CostEstimate(
        flops=2 * tasks * width**3, bytes_accessed=2 * tasks * width**2, transcendentals=0
    )
    if loading:
        return pl.pallas_call(
            functools.partial(loading_kernel, slots // 2),
            out_shape=total,
            in_specs=[SMEM, SMEM, VMEM, HBM, HBM],
            out_specs=VMEM,
            scratch_shapes=[
                pltpu.VMEM(left.shape, BF16),
                pltpu.VMEM(left.shape, BF16),
                pltpu.SemaphoreType.DMA((2, tasks)),
            ],
            compiler_params=room(47),
            cost_estimate=cost,
            name="loading",
        )(targets, core, vector, left, right)
    return pl.pallas_call(
        functools.partial(resident_kernel, slots // 2),
        out_shape=total,
        in_specs=[SMEM, SMEM, VMEM, VMEM, VMEM],
        out_specs=VMEM,
        compiler_params=room(4),
        cost_estimate=cost,
        name="resident",
    )(targets, core, vector, left, right)


def pack_kernel(kept, arrived, packed):
    slots, width, _ = kept.shape
    owners, halves, local_sectors, rows, _ = packed.shape
    for slot in range(slots):

        def one_owner(owner, carry, slot=slot):
            here = pl.ds(pl.multiple_of(owner * rows, rows), rows)
            total = kept[slot, here, :] + arrived[slot, here, :]
            packed[owner, slot // local_sectors, slot % local_sectors] = total.astype(BF16)
            return carry

        lax.fori_loop(0, owners, one_owner, 0, unroll=4)


def pack(kept, arrived, owners):
    slots, width, _ = kept.shape
    return pl.pallas_call(
        pack_kernel,
        out_shape=jax.ShapeDtypeStruct((owners, 2, slots // 2, width // owners, width), BF16),
        in_specs=[VMEM, VMEM],
        out_specs=VMEM,
        compiler_params=room(4),
        name="pack",
    )(kept, arrived)


def summed(pieces):
    shape = pieces.shape[1:]
    count = pieces.shape[0]

    def add(index, total):
        return total + pieces[index].astype(F32)

    return lax.fori_loop(0, count, add, jnp.zeros(shape, F32), unroll=8)


def lanes(value):
    local_sectors, rows, width = value.shape
    flat = jnp.sum(value.reshape(local_sectors * rows, width), axis=0, keepdims=True)
    return sum(flat[:, at : at + 128] for at in range(0, width, 128))


def first_kernel(offset, pieces, wave, precond, sigma, sums):
    rows = precond.shape[1]
    own = wave[:, pl.ds(pl.multiple_of(offset[0], rows), rows), :].astype(F32)
    total = summed(pieces)
    sigma[...] = total
    ratio, scaled = total / precond[...], own / precond[...]
    terms = (
        own * own,
        own * total,
        own * ratio,
        own * scaled,
        ratio * ratio,
        ratio * scaled,
        scaled * scaled,
    )
    one = jnp.concatenate([lanes(term) for term in terms] + [jnp.zeros((1, 128), F32)], axis=0)
    sums[...] = jnp.broadcast_to(one[None], sums.shape)


def second_kernel(offset, sums, sigma, wave, precond, copies):
    rows = precond.shape[1]
    own = wave[:, pl.ds(pl.multiple_of(offset[0], rows), rows), :].astype(F32)
    whole = jnp.sum(summed(sums), axis=1, keepdims=True)
    norm_sq, w_s, w_r, w_b, r_r, r_b, b_b = (whole[k : k + 1] for k in range(7))
    shift = w_s / norm_sq - 1.0
    projected = w_r - shift * w_b
    correction_sq = r_r - 2.0 * shift * r_b + shift * shift * b_b
    along = projected / norm_sq
    update_sq = correction_sq - projected * along
    scale = jnp.sqrt(norm_sq) * lax.rsqrt(update_sq + 1e-06)
    correction = (sigma[...] - shift[None] * own) / precond[...]
    new = ((correction - along[None] * own) * scale[None]).astype(BF16)
    copies[...] = jnp.broadcast_to(new[None], copies.shape)


def sum_kernel(pieces, sigma):
    sigma[...] = summed(pieces)


def on_device(wavefunction, left_blocks, right_blocks, target_sector, preconditioner):
    local_sectors, width, _ = wavefunction.shape
    rows = preconditioner.shape[1]
    owners = lax.axis_size(OP)
    offset = (lax.axis_index(OP) * rows).reshape(1)
    mine = lax.axis_index(CORE).reshape(1)
    targets = target_sector.reshape(-1)
    row_shape = jax.ShapeDtypeStruct((local_sectors, rows, width), F32)

    def partial_pieces(vector, left, right, loading):
        sent = apply_terms(targets, 1 - mine, vector, left, right, loading)
        arrived = lax.ppermute(sent, CORE, [(0, 1), (1, 0)])
        kept = apply_terms(targets, mine, vector, left, right, loading)
        packed = pack(kept, arrived, owners)
        pieces = packed.reshape(2 * owners, local_sectors, rows, width)
        return exchange(pieces, CHIPS)

    left, right = (
        blocks.reshape(-1, width, width) for blocks in (left_blocks, right_blocks)
    )
    pieces = partial_pieces(wavefunction, left, right, True)
    devices = lax.axis_size(EVERY)
    sigma_first, sums = pl.pallas_call(
        first_kernel,
        out_shape=(row_shape, jax.ShapeDtypeStruct((devices, 8, 128), F32)),
        in_specs=[SMEM, VMEM, VMEM, VMEM],
        out_specs=(VMEM, VMEM),
        compiler_params=room(4),
        name="first",
    )(offset, pieces, wavefunction, preconditioner)
    sums = exchange(sums, EVERY)
    copies = pl.pallas_call(
        second_kernel,
        out_shape=jax.ShapeDtypeStruct((owners, local_sectors, rows, width), BF16),
        in_specs=[SMEM, VMEM, VMEM, VMEM, VMEM],
        out_specs=VMEM,
        compiler_params=room(4),
        name="second",
    )(offset, sums, sigma_first, wavefunction, preconditioner)
    pieces = partial_pieces(exchange(copies, OP), left, right, False)
    sigma_second = pl.pallas_call(
        sum_kernel,
        out_shape=row_shape,
        in_specs=[VMEM],
        out_specs=VMEM,
        compiler_params=room(4),
        name="last",
    )(pieces)
    return (sigma_first, sigma_second)


def solution(mesh):
    torus = Mesh(mesh.devices.reshape(2, 4, 4, 2, 2), EVERY)
    placed = (
        P(SECTOR, None, None),
        P(OP, SECTOR, None, None),
        P(OP, SECTOR, None, None),
        P(OP, SECTOR),
        P(SECTOR, OP, None),
    )
    return jax.shard_map(
        on_device,
        mesh=torus,
        in_specs=placed,
        out_specs=(P(SECTOR, OP, None), P(SECTOR, OP, None)),
        check_vma=False,
    )
```

```python
import functools

import jax
import jax.numpy as jnp
from jax import lax
from jax.experimental import pallas as pl
from jax.experimental.pallas import tpu as pltpu
from jax.sharding import Mesh
from jax.sharding import PartitionSpec as P

SECTOR = ("sector_0", "sector_1")
OP = ("op_0", "op_1", "op_2")
CHIPS = ("op_0", "op_1", "op_2", "sector_0")
EVERY = ("op_0", "op_1", "op_2", "sector_0", "sector_1")
CORE = "sector_1"
F32 = jnp.float32
BF16 = jnp.bfloat16
VMEM = pl.BlockSpec(memory_space=pltpu.VMEM)
SMEM = pl.BlockSpec(memory_space=pltpu.SMEM)
HBM = pl.BlockSpec(memory_space=pltpu.HBM)


def room(mebibytes):
    return pltpu.CompilerParams(vmem_limit_bytes=mebibytes * 2**20)


def exchange(pieces, axis):
    return lax.all_to_all(pieces, axis, split_axis=0, concat_axis=0, tiled=True)


def wanted(targets, core, task):
    local_sectors = targets.shape[0]
    target = targets[lax.rem(task, local_sectors), task // local_sectors]
    return target, lax.rem(target // local_sectors, 2) == core[0]


def all_tasks(targets, core, source, lefts, rights, totals, touched, arrive):
    local_sectors = targets.shape[0]
    slots, width, _ = totals.shape
    for slot in range(slots):
        touched[slot] = 0

    def one_task(task, carry):
        target, chosen = wanted(targets, core, task)

        @pl.when(chosen)
        def _():
            slot = target // (2 * local_sectors) * local_sectors + lax.rem(target, local_sectors)
            fresh = touched[slot] == 0
            touched[slot] = 1
            arrive(task)
            middle = jnp.dot(
                lefts[task], source(lax.rem(task, local_sectors)), preferred_element_type=F32
            ).astype(BF16)
            share = lax.dot_general(
                middle, rights[task], (((1,), (1,)), ((), ())), preferred_element_type=F32
            )
            totals[slot] = share + jnp.where(fresh, 0.0, totals[slot])

        return carry

    lax.fori_loop(0, lefts.shape[0], one_task, 0)
    for slot in range(slots):

        @pl.when(touched[slot] == 0)
        def _(slot=slot):
            totals[slot] = jnp.zeros((width, width), F32)


def loading_kernel(
    targets, core, vector, left, right, totals, lefts, rights, touched, sems
):
    def copies(task):
        return (
            pltpu.make_async_copy(left.at[task], lefts.at[task], sems.at[0, task]),
            pltpu.make_async_copy(right.at[task], rights.at[task], sems.at[1, task]),
        )

    def start(task, carry):
        @pl.when(wanted(targets, core, task)[1])
        def _():
            for copy in copies(task):
                copy.start()

        return carry

    def arrive(task):
        for copy in copies(task):
            copy.wait()

    lax.fori_loop(0, left.shape[0], start, 0)
    all_tasks(
        targets, core, lambda sector: vector[sector], lefts, rights, totals, touched, arrive
    )


def resident_kernel(targets, core, vector, lefts, rights, totals, touched):
    width = lefts.shape[1]

    def source(sector):
        return vector[:, sector].reshape(width, width)

    all_tasks(targets, core, source, lefts, rights, totals, touched, lambda task: None)


def apply_terms(targets, core, vector, left, right, loading, grant):
    tasks, width, _ = left.shape
    slots = tasks // 2
    flags = pltpu.SMEM((slots,), jnp.int32)
    scratch = [flags]
    if loading:
        scratch = [
            pltpu.VMEM(left.shape, BF16),
            pltpu.VMEM(left.shape, BF16),
            flags,
            pltpu.SemaphoreType.DMA((2, tasks)),
        ]
    return pl.pallas_call(
        loading_kernel if loading else resident_kernel,
        out_shape=jax.ShapeDtypeStruct((slots, width, width), F32),
        in_specs=[SMEM, SMEM] + [VMEM] + [HBM if loading else VMEM] * 2,
        out_specs=VMEM,
        scratch_shapes=scratch,
        compiler_params=room(grant),
        cost_estimate=pl.CostEstimate(
            flops=2 * tasks * width**3, bytes_accessed=2 * tasks * width**2, transcendentals=0
        ),
        name="loading" if loading else "resident",
    )(targets, core, vector, left, right)


def pack_kernel(kept, arrived, packed):
    slots, width, _ = kept.shape
    owners, halves, local_sectors, rows, _ = packed.shape
    for slot in range(slots):

        def one_owner(owner, carry, slot=slot):
            here = pl.ds(pl.multiple_of(owner * rows, rows), rows)
            total = kept[slot, here, :] + arrived[slot, here, :].astype(F32)
            packed[owner, slot // local_sectors, slot % local_sectors] = total.astype(BF16)
            return carry

        lax.fori_loop(0, owners, one_owner, 0, unroll=4)


def pack(kept, arrived, owners):
    slots, width, _ = kept.shape
    return pl.pallas_call(
        pack_kernel,
        out_shape=jax.ShapeDtypeStruct((owners, 2, slots // 2, width // owners, width), BF16),
        in_specs=[VMEM, VMEM],
        out_specs=VMEM,
        compiler_params=room(4),
        name="pack",
    )(kept, arrived)


def summed(pieces):
    shape = pieces.shape[1:]
    count = pieces.shape[0]

    def add(index, total):
        return total + pieces[index].astype(F32)

    return lax.fori_loop(0, count, add, jnp.zeros(shape, F32), unroll=8)


def lanes(value):
    local_sectors, rows, width = value.shape
    flat = jnp.sum(value.reshape(local_sectors * rows, width), axis=0, keepdims=True)
    return sum(flat[:, at : at + 128] for at in range(0, width, 128))


def first_kernel(offset, pieces, wave, precond, sigma, again, sums):
    rows = precond.shape[1]
    own = wave[:, pl.ds(pl.multiple_of(offset[0], rows), rows), :].astype(F32)
    total = summed(pieces)
    sigma[...] = total
    again[...] = total
    ratio, scaled = total / precond[...], own / precond[...]
    terms = (
        own * own,
        own * total,
        own * ratio,
        own * scaled,
        ratio * ratio,
        ratio * scaled,
        scaled * scaled,
    )
    one = jnp.concatenate([lanes(term) for term in terms] + [jnp.zeros((1, 128), F32)], axis=0)
    one = jnp.sum(one, axis=1, keepdims=True)
    row = lax.broadcasted_iota(jnp.int32, (8, 128), 0)
    lane = lax.broadcasted_iota(jnp.int32, (8, 128), 1)
    one = jnp.sum(jnp.where(row == lane, one, 0.0), axis=0, keepdims=True)
    sums[...] = jnp.broadcast_to(one[None], sums.shape)


def second_kernel(offset, sums, sigma, wave, precond, copies):
    rows = precond.shape[1]
    own = wave[:, pl.ds(pl.multiple_of(offset[0], rows), rows), :].astype(F32)
    whole = summed(sums)
    norm_sq, w_s, w_r, w_b, r_r, r_b, b_b = (whole[:, k : k + 1] for k in range(7))
    shift = w_s / norm_sq - 1.0
    projected = w_r - shift * w_b
    correction_sq = r_r - 2.0 * shift * r_b + shift * shift * b_b
    along = projected / norm_sq
    update_sq = correction_sq - projected * along
    scale = jnp.sqrt(norm_sq) * lax.rsqrt(update_sq + 1e-06)
    correction = (sigma[...] - shift[None] * own) / precond[...]
    new = ((correction - along[None] * own) * scale[None]).astype(BF16)
    copies[...] = jnp.broadcast_to(new[None], copies.shape)


def sum_kernel(pieces, sigma):
    sigma[...] = summed(pieces)


def on_device(wavefunction, left_blocks, right_blocks, target_sector, preconditioner):
    local_sectors, width, _ = wavefunction.shape
    rows = preconditioner.shape[1]
    owners = lax.axis_size(OP)
    offset = (lax.axis_index(OP) * rows).reshape(1)
    mine = lax.axis_index(CORE).reshape(1)
    theirs = 1 - mine
    targets = target_sector.T
    left, right = (
        blocks.reshape(-1, width, width) for blocks in (left_blocks, right_blocks)
    )
    row_shape = jax.ShapeDtypeStruct((local_sectors, rows, width), F32)
    offset, mine, theirs = lax.optimization_barrier((offset, mine, theirs))

    def partial_pieces(vector, loading):
        sent = apply_terms(targets, theirs, vector, left, right, loading, 47 if loading else 4)
        arrived = lax.ppermute(sent, CORE, [(0, 1), (1, 0)])
        kept = apply_terms(targets, mine, vector, left, right, loading, 47 if loading else 4)
        packed = pack(kept, arrived, owners)
        return exchange(packed.reshape(2 * owners, local_sectors, rows, width), CHIPS)

    pieces = partial_pieces(wavefunction, True)
    devices = lax.axis_size(EVERY)
    sigma_first, again, sums = pl.pallas_call(
        first_kernel,
        out_shape=(row_shape, row_shape, jax.ShapeDtypeStruct((devices, 1, 128), F32)),
        in_specs=[SMEM, VMEM, VMEM, VMEM],
        out_specs=(VMEM, VMEM, VMEM),
        compiler_params=room(4),
        name="first",
    )(offset, pieces, wavefunction, preconditioner)
    sums = exchange(sums, EVERY)
    copies = pl.pallas_call(
        second_kernel,
        out_shape=jax.ShapeDtypeStruct((owners, local_sectors, rows, width), BF16),
        in_specs=[SMEM, VMEM, VMEM, VMEM, VMEM],
        out_specs=VMEM,
        compiler_params=room(4),
        name="second",
    )(offset, sums, again, wavefunction, preconditioner)
    pieces = partial_pieces(exchange(copies, OP), False)
    sigma_second = pl.pallas_call(
        sum_kernel,
        out_shape=row_shape,
        in_specs=[VMEM],
        out_specs=VMEM,
        compiler_params=room(4),
        name="last",
    )(pieces)
    return (sigma_first, sigma_second)


def solution(mesh):
    torus = Mesh(mesh.devices.reshape(2, 4, 4, 2, 2), EVERY)
    placed = (
        P(SECTOR, None, None),
        P(OP, SECTOR, None, None),
        P(OP, SECTOR, None, None),
        P(OP, SECTOR),
        P(SECTOR, OP, None),
    )
    return jax.shard_map(
        on_device,
        mesh=torus,
        in_specs=placed,
        out_specs=(P(SECTOR, OP, None), P(SECTOR, OP, None)),
        check_vma=False,
    )
```

```python
import functools

import jax
import jax.numpy as jnp
from jax import lax
from jax.experimental import pallas as pl
from jax.experimental.pallas import tpu as pltpu
from jax.sharding import Mesh
from jax.sharding import PartitionSpec as P

SECTOR = ("sector_0", "sector_1")
OP = ("op_0", "op_1", "op_2")
CHIPS = ("op_0", "op_1", "op_2", "sector_0")
EVERY = ("op_0", "op_1", "op_2", "sector_0", "sector_1")
CORE = "sector_1"
F32 = jnp.float32
BF16 = jnp.bfloat16
VMEM = pl.BlockSpec(memory_space=pltpu.VMEM)
SMEM = pl.BlockSpec(memory_space=pltpu.SMEM)
HBM = pl.BlockSpec(memory_space=pltpu.HBM)


def room(mebibytes):
    return pltpu.CompilerParams(vmem_limit_bytes=mebibytes * 2**20)


def exchange(pieces, axis):
    return lax.all_to_all(pieces, axis, split_axis=0, concat_axis=0, tiled=True)


def chosen_tasks(targets, core, order):
    local_sectors, terms = targets.shape

    def scan(task, count):
        target = targets[lax.rem(task, local_sectors), task // local_sectors]
        order[count] = task
        return count + (lax.rem(target // local_sectors, 2) == core[0]).astype(jnp.int32)

    return lax.fori_loop(0, local_sectors * terms, scan, jnp.int32(0))


def run_tasks(targets, order, count, source, lefts, rights, totals, touched, arrive):
    local_sectors = targets.shape[0]
    slots, width, _ = totals.shape
    for slot in range(slots):
        touched[slot] = 0

    def middle_of(task):
        vector = source(lax.rem(task, local_sectors))
        return jnp.dot(lefts[task], vector, preferred_element_type=F32).astype(BF16)

    def add(task, middle):
        target = targets[lax.rem(task, local_sectors), task // local_sectors]
        slot = target // (2 * local_sectors) * local_sectors + lax.rem(target, local_sectors)
        fresh = touched[slot] == 0
        touched[slot] = 1
        share = lax.dot_general(
            middle, rights[task], (((1,), (1,)), ((), ())), preferred_element_type=F32
        )
        totals[slot] = share + jnp.where(fresh, 0.0, totals[slot])

    def pair(index, carry):
        tasks = order[2 * index], order[2 * index + 1]
        for task in tasks:
            arrive(task)
        for task, middle in zip(tasks, [middle_of(task) for task in tasks]):
            add(task, middle)
        return carry

    lax.fori_loop(0, count // 2, pair, 0)

    @pl.when(lax.rem(count, 2) == 1)
    def _():
        task = order[count - 1]
        arrive(task)
        add(task, middle_of(task))

    for slot in range(slots):

        @pl.when(touched[slot] == 0)
        def _(slot=slot):
            totals[slot] = jnp.zeros((width, width), F32)


def apply_kernel(loading, sending, *refs):
    targets, core, vector, left, right, out, touched, order = refs[:8]
    rest = list(refs[8:])
    totals = rest.pop(0) if sending else out
    count = chosen_tasks(targets, core, order)
    if loading:
        lefts, rights, sems = rest

        def copies(task):
            return (
                pltpu.make_async_copy(left.at[task], lefts.at[task], sems.at[0, task]),
                pltpu.make_async_copy(right.at[task], rights.at[task], sems.at[1, task]),
            )

        def start(index, carry):
            for copy in copies(order[index]):
                copy.start()
            return carry

        def arrive(task):
            for copy in copies(task):
                copy.wait()

        lax.fori_loop(0, count, start, 0)
    else:
        lefts, rights = left, right

        def arrive(task):
            del task

    width = lefts.shape[1]

    def source(sector):
        if loading:
            return vector[sector]
        return vector[:, sector].reshape(width, width)

    run_tasks(targets, order, count, source, lefts, rights, totals, touched, arrive)
    if sending:
        out[...] = totals[...].astype(BF16)


def apply_terms(targets, core, vector, left, right, loading, sending):
    tasks, width, _ = left.shape
    slots = tasks // 2
    scratch = [pltpu.SMEM((slots,), jnp.int32), pltpu.SMEM((tasks + 1,), jnp.int32)]
    if sending:
        scratch += [pltpu.VMEM((slots, width, width), F32)]
    if loading:
        scratch += [
            pltpu.VMEM(left.shape, BF16),
            pltpu.VMEM(left.shape, BF16),
            pltpu.SemaphoreType.DMA((2, tasks)),
        ]
    return pl.pallas_call(
        functools.partial(apply_kernel, loading, sending),
        out_shape=jax.ShapeDtypeStruct((slots, width, width), BF16 if sending else F32),
        in_specs=[SMEM, SMEM, VMEM] + [HBM if loading else VMEM] * 2,
        out_specs=VMEM,
        scratch_shapes=scratch,
        compiler_params=room((50 if sending else 46) if loading else 8),
        cost_estimate=pl.CostEstimate(
            flops=2 * tasks * width**3, bytes_accessed=2 * tasks * width**2, transcendentals=0
        ),
        name=("load_" if loading else "") + ("send" if sending else "keep"),
    )(targets, core, vector, left, right)


def pack_kernel(kept, arrived, packed):
    slots, width, _ = kept.shape
    owners, halves, local_sectors, rows, _ = packed.shape
    for slot in range(slots):

        def one_owner(owner, carry, slot=slot):
            here = pl.ds(pl.multiple_of(owner * rows, rows), rows)
            total = kept[slot, here, :] + arrived[slot, here, :].astype(F32)
            packed[owner, slot // local_sectors, slot % local_sectors] = total.astype(BF16)
            return carry

        lax.fori_loop(0, owners, one_owner, 0, unroll=4)


def pack(kept, arrived, owners):
    slots, width, _ = kept.shape
    return pl.pallas_call(
        pack_kernel,
        out_shape=jax.ShapeDtypeStruct((owners, 2, slots // 2, width // owners, width), BF16),
        in_specs=[VMEM, VMEM],
        out_specs=VMEM,
        compiler_params=room(4),
        name="pack",
    )(kept, arrived)


def summed(pieces):
    shape = pieces.shape[1:]
    count = pieces.shape[0]

    def add(index, total):
        return total + pieces[index].astype(F32)

    return lax.fori_loop(0, count, add, jnp.zeros(shape, F32), unroll=8)


def lanes(value):
    local_sectors, rows, width = value.shape
    flat = jnp.sum(value.reshape(local_sectors * rows, width), axis=0, keepdims=True)
    return sum(flat[:, at : at + 128] for at in range(0, width, 128))


def first_kernel(offset, pieces, wave, precond, sigma, again, sums):
    rows = precond.shape[1]
    own = wave[:, pl.ds(pl.multiple_of(offset[0], rows), rows), :].astype(F32)
    total = summed(pieces)
    sigma[...] = total
    again[...] = total
    ratio, scaled = total / precond[...], own / precond[...]
    terms = (
        own * own,
        own * total,
        own * ratio,
        own * scaled,
        ratio * ratio,
        ratio * scaled,
        scaled * scaled,
    )
    one = jnp.concatenate([lanes(term) for term in terms] + [jnp.zeros((1, 128), F32)], axis=0)
    one = jnp.sum(one, axis=1, keepdims=True)
    row = lax.broadcasted_iota(jnp.int32, (8, 128), 0)
    lane = lax.broadcasted_iota(jnp.int32, (8, 128), 1)
    one = jnp.sum(jnp.where(row == lane, one, 0.0), axis=0, keepdims=True)
    sums[...] = jnp.broadcast_to(one[None], sums.shape)


def second_kernel(offset, sums, sigma, wave, precond, copies):
    rows = precond.shape[1]
    own = wave[:, pl.ds(pl.multiple_of(offset[0], rows), rows), :].astype(F32)
    whole = summed(sums)
    norm_sq, w_s, w_r, w_b, r_r, r_b, b_b = (whole[:, k : k + 1] for k in range(7))
    shift = w_s / norm_sq - 1.0
    projected = w_r - shift * w_b
    correction_sq = r_r - 2.0 * shift * r_b + shift * shift * b_b
    along = projected / norm_sq
    update_sq = correction_sq - projected * along
    scale = jnp.sqrt(norm_sq) * lax.rsqrt(update_sq + 1e-06)
    correction = (sigma[...] - shift[None] * own) / precond[...]
    new = ((correction - along[None] * own) * scale[None]).astype(BF16)
    copies[...] = jnp.broadcast_to(new[None], copies.shape)


def sum_kernel(pieces, sigma):
    sigma[...] = summed(pieces)


def on_device(wavefunction, left_blocks, right_blocks, target_sector, preconditioner):
    local_sectors, width, _ = wavefunction.shape
    rows = preconditioner.shape[1]
    owners = lax.axis_size(OP)
    offset = (lax.axis_index(OP) * rows).reshape(1)
    mine = lax.axis_index(CORE).reshape(1)
    theirs = 1 - mine
    targets = target_sector.T
    left, right = (
        blocks.reshape(-1, width, width) for blocks in (left_blocks, right_blocks)
    )
    row_shape = jax.ShapeDtypeStruct((local_sectors, rows, width), F32)
    offset, mine, theirs = lax.optimization_barrier((offset, mine, theirs))

    def partial_pieces(vector, loading):
        sent = apply_terms(targets, theirs, vector, left, right, loading, True)
        arrived = lax.ppermute(sent, CORE, [(0, 1), (1, 0)])
        kept = apply_terms(targets, mine, vector, left, right, loading, False)
        packed = pack(kept, arrived, owners)
        return exchange(packed.reshape(2 * owners, local_sectors, rows, width), CHIPS)

    pieces = partial_pieces(wavefunction, True)
    devices = lax.axis_size(EVERY)
    sigma_first, again, sums = pl.pallas_call(
        first_kernel,
        out_shape=(row_shape, row_shape, jax.ShapeDtypeStruct((devices, 1, 128), F32)),
        in_specs=[SMEM, VMEM, VMEM, VMEM],
        out_specs=(VMEM, VMEM, VMEM),
        compiler_params=room(4),
        name="first",
    )(offset, pieces, wavefunction, preconditioner)
    sums = exchange(sums, EVERY)
    copies = pl.pallas_call(
        second_kernel,
        out_shape=jax.ShapeDtypeStruct((owners, local_sectors, rows, width), BF16),
        in_specs=[SMEM, VMEM, VMEM, VMEM, VMEM],
        out_specs=VMEM,
        compiler_params=room(4),
        name="second",
    )(offset, sums, again, wavefunction, preconditioner)
    pieces = partial_pieces(exchange(copies, OP), False)
    sigma_second = pl.pallas_call(
        sum_kernel,
        out_shape=row_shape,
        in_specs=[VMEM],
        out_specs=VMEM,
        compiler_params=room(4),
        name="last",
    )(pieces)
    return (sigma_first, sigma_second)


def solution(mesh):
    torus = Mesh(mesh.devices.reshape(2, 4, 4, 2, 2), EVERY)
    placed = (
        P(SECTOR, None, None),
        P(OP, SECTOR, None, None),
        P(OP, SECTOR, None, None),
        P(OP, SECTOR),
        P(SECTOR, OP, None),
    )
    return jax.shard_map(
        on_device,
        mesh=torus,
        in_specs=placed,
        out_specs=(P(SECTOR, OP, None), P(SECTOR, OP, None)),
        check_vma=False,
    )
```

```python
import functools
import itertools

import jax
import jax.numpy as jnp
from jax import lax
from jax.experimental import pallas as pl
from jax.experimental.pallas import tpu as pltpu
from jax.sharding import Mesh
from jax.sharding import PartitionSpec as P

SECTOR = ("sector_0", "sector_1")
OP = ("op_0", "op_1", "op_2")
EVERY = ("op_0", "op_1", "op_2", "sector_0", "sector_1")
CORE = "sector_1"
F32 = jnp.float32
BF16 = jnp.bfloat16
VMEM = pl.BlockSpec(memory_space=pltpu.VMEM)
SMEM = pl.BlockSpec(memory_space=pltpu.SMEM)
HBM = pl.BlockSpec(memory_space=pltpu.HBM)


def room(mebibytes):
    return pltpu.CompilerParams(vmem_limit_bytes=mebibytes * 2**20)


def exchange(pieces, axis):
    return lax.all_to_all(pieces, axis, split_axis=0, concat_axis=0, tiled=True)


def chosen_tasks(targets, core, order):
    local_sectors, terms = targets.shape

    def scan(task, count):
        target = targets[lax.rem(task, local_sectors), task // local_sectors]
        order[count] = task
        return count + (lax.rem(target // local_sectors, 2) == core[0]).astype(jnp.int32)

    return lax.fori_loop(0, local_sectors * terms, scan, jnp.int32(0))


def run_tasks(targets, order, count, source, lefts, rights, totals, touched, arrive):
    local_sectors = targets.shape[0]
    slots, width, _ = totals.shape
    for slot in range(slots):
        touched[slot] = 0

    def middle_of(task):
        vector = source(lax.rem(task, local_sectors))
        return jnp.dot(lefts[task], vector, preferred_element_type=F32).astype(BF16)

    def add(task, middle):
        target = targets[lax.rem(task, local_sectors), task // local_sectors]
        slot = target // (2 * local_sectors) * local_sectors + lax.rem(target, local_sectors)
        fresh = touched[slot] == 0
        touched[slot] = 1
        share = lax.dot_general(
            middle, rights[task], (((1,), (1,)), ((), ())), preferred_element_type=F32
        )
        totals[slot] = share + jnp.where(fresh, 0.0, totals[slot])

    def pair(index, carry):
        tasks = order[2 * index], order[2 * index + 1]
        for task in tasks:
            arrive(task)
        for task, middle in zip(tasks, [middle_of(task) for task in tasks]):
            add(task, middle)
        return carry

    lax.fori_loop(0, count // 2, pair, 0)

    @pl.when(lax.rem(count, 2) == 1)
    def _():
        task = order[count - 1]
        arrive(task)
        add(task, middle_of(task))

    for slot in range(slots):

        @pl.when(touched[slot] == 0)
        def _(slot=slot):
            totals[slot] = jnp.zeros((width, width), F32)


def apply_kernel(loading, sending, *refs):
    targets, core, vector, left, right, out, touched, order = refs[:8]
    rest = list(refs[8:])
    totals = rest.pop(0) if sending else out
    count = chosen_tasks(targets, core, order)
    if loading:
        lefts, rights, sems = rest

        def copies(task):
            return (
                pltpu.make_async_copy(left.at[task], lefts.at[task], sems.at[0, task]),
                pltpu.make_async_copy(right.at[task], rights.at[task], sems.at[1, task]),
            )

        def start(index, carry):
            for copy in copies(order[index]):
                copy.start()
            return carry

        def arrive(task):
            for copy in copies(task):
                copy.wait()

        lax.fori_loop(0, count, start, 0)
    else:
        lefts, rights = left, right

        def arrive(task):
            del task

    width = lefts.shape[1]

    def source(sector):
        if loading:
            return vector[sector]
        return vector[:, sector].reshape(width, width)

    run_tasks(targets, order, count, source, lefts, rights, totals, touched, arrive)
    if sending:
        out[...] = totals[...].astype(BF16)


def apply_terms(targets, core, vector, left, right, loading, sending):
    tasks, width, _ = left.shape
    slots = tasks // 2
    scratch = [pltpu.SMEM((slots,), jnp.int32), pltpu.SMEM((tasks + 1,), jnp.int32)]
    if sending:
        scratch += [pltpu.VMEM((slots, width, width), F32)]
    if loading:
        scratch += [
            pltpu.VMEM(left.shape, BF16),
            pltpu.VMEM(left.shape, BF16),
            pltpu.SemaphoreType.DMA((2, tasks)),
        ]
    return pl.pallas_call(
        functools.partial(apply_kernel, loading, sending),
        out_shape=jax.ShapeDtypeStruct((slots, width, width), BF16 if sending else F32),
        in_specs=[SMEM, SMEM, VMEM] + [HBM if loading else VMEM] * 2,
        out_specs=VMEM,
        scratch_shapes=scratch,
        compiler_params=room((50 if sending else 46) if loading else 8),
        cost_estimate=pl.CostEstimate(
            flops=2 * tasks * width**3, bytes_accessed=2 * tasks * width**2, transcendentals=0
        ),
        name=("load_" if loading else "") + ("send" if sending else "keep"),
    )(targets, core, vector, left, right)


def place(op_0, op_1, op_2, half, core):
    return (((op_0 * 4 + op_1) * 4 + op_2) * 2 + half) * 2 + core


def along_ring(value, step):
    pairs = []
    for op_0, op_1, op_2, half in itertools.product(range(2), range(4), range(4), range(2)):
        first, second = (op_1 + step) % 4, (op_2 + step) % 4
        pairs.append((place(op_0, op_1, op_2, half, 0), place(op_0, first, op_2, half, 0)))
        pairs.append((place(op_0, op_1, op_2, half, 1), place(op_0, op_1, second, half, 1)))
    return lax.ppermute(value, EVERY, pairs)


def across_rings(pieces):
    rest = list(itertools.product(range(2), range(4), range(2)))
    groups = [[place(low, ring, at, half, 0) for low, at, half in rest] for ring in range(4)]
    groups += [[place(low, at, ring, half, 1) for low, at, half in rest] for ring in range(4)]
    return lax.all_to_all(
        pieces, EVERY, split_axis=0, concat_axis=0, axis_index_groups=groups, tiled=True
    )


def pack_kernel(ring, core, kept, arrived, own, *sent):
    others, local_sectors, rows, _ = own.shape

    def one_block(index, carry):
        other, sector = index // local_sectors, lax.rem(index, local_sectors)
        low, at, half = other // 8, lax.rem(other // 2, 4), lax.rem(other, 2)
        slot = half * local_sectors + sector
        for step in range(4):
            to = lax.rem(ring[0] + step, 4)
            block = low * 16 + jnp.where(core[0] == 0, to * 4 + at, at * 4 + to)
            here = pl.ds(pl.multiple_of(block * rows, rows), rows)
            total = kept[slot, here, :] + arrived[slot, here, :].astype(F32)
            if step == 0:
                own[other, sector] = total
            else:
                sent[step - 1][other, sector] = total.astype(BF16)
        return carry

    lax.fori_loop(0, others * local_sectors, one_block, 0, unroll=2)


def pack(ring, core, kept, arrived, shape):
    return pl.pallas_call(
        pack_kernel,
        out_shape=[jax.ShapeDtypeStruct(shape, F32)] + [jax.ShapeDtypeStruct(shape, BF16)] * 3,
        in_specs=[SMEM, SMEM, VMEM, VMEM],
        out_specs=[VMEM] * 4,
        compiler_params=room(4),
        name="pack",
    )(ring, core, kept, arrived)


def meet_kernel(own, first, second, third, out):
    def one(index, carry):
        total = own[index] + first[index].astype(F32)
        total += second[index].astype(F32) + third[index].astype(F32)
        out[index] = total.astype(BF16)
        return carry

    lax.fori_loop(0, own.shape[0], one, 0, unroll=4)


def meet(own, arrived):
    return pl.pallas_call(
        meet_kernel,
        out_shape=jax.ShapeDtypeStruct(own.shape, BF16),
        in_specs=[VMEM] * 4,
        out_specs=VMEM,
        compiler_params=room(4),
        name="meet",
    )(own, *arrived)


def summed(pieces):
    shape = pieces.shape[1:]
    count = pieces.shape[0]

    def add(index, total):
        return total + pieces[index].astype(F32)

    return lax.fori_loop(0, count, add, jnp.zeros(shape, F32), unroll=8)


def lanes(value):
    local_sectors, rows, width = value.shape
    flat = jnp.sum(value.reshape(local_sectors * rows, width), axis=0, keepdims=True)
    return sum(flat[:, at : at + 128] for at in range(0, width, 128))


def first_kernel(offset, pieces, wave, precond, sigma, again, sums):
    rows = precond.shape[1]
    own = wave[:, pl.ds(pl.multiple_of(offset[0], rows), rows), :].astype(F32)
    total = summed(pieces)
    sigma[...] = total
    again[...] = total
    ratio, scaled = total / precond[...], own / precond[...]
    terms = (
        own * own,
        own * total,
        own * ratio,
        own * scaled,
        ratio * ratio,
        ratio * scaled,
        scaled * scaled,
    )
    one = jnp.concatenate([lanes(term) for term in terms] + [jnp.zeros((1, 128), F32)], axis=0)
    one = jnp.sum(one, axis=1, keepdims=True)
    row = lax.broadcasted_iota(jnp.int32, (8, 128), 0)
    lane = lax.broadcasted_iota(jnp.int32, (8, 128), 1)
    one = jnp.sum(jnp.where(row == lane, one, 0.0), axis=0, keepdims=True)
    sums[...] = jnp.broadcast_to(one[None], sums.shape)


def second_kernel(offset, sums, sigma, wave, precond, copies):
    rows = precond.shape[1]
    own = wave[:, pl.ds(pl.multiple_of(offset[0], rows), rows), :].astype(F32)
    whole = summed(sums)
    norm_sq, w_s, w_r, w_b, r_r, r_b, b_b = (whole[:, k : k + 1] for k in range(7))
    shift = w_s / norm_sq - 1.0
    projected = w_r - shift * w_b
    correction_sq = r_r - 2.0 * shift * r_b + shift * shift * b_b
    along = projected / norm_sq
    update_sq = correction_sq - projected * along
    scale = jnp.sqrt(norm_sq) * lax.rsqrt(update_sq + 1e-06)
    correction = (sigma[...] - shift[None] * own) / precond[...]
    new = ((correction - along[None] * own) * scale[None]).astype(BF16)
    copies[...] = jnp.broadcast_to(new[None], copies.shape)


def sum_kernel(pieces, sigma):
    sigma[...] = summed(pieces)


def on_device(wavefunction, left_blocks, right_blocks, target_sector, preconditioner):
    local_sectors, width, _ = wavefunction.shape
    rows = preconditioner.shape[1]
    owners = lax.axis_size(OP)
    offset = (lax.axis_index(OP) * rows).reshape(1)
    mine = lax.axis_index(CORE).reshape(1)
    theirs = 1 - mine
    ring = jnp.where(mine == 0, lax.axis_index("op_1"), lax.axis_index("op_2"))
    targets = target_sector.T
    left, right = (
        blocks.reshape(-1, width, width) for blocks in (left_blocks, right_blocks)
    )
    row_shape = jax.ShapeDtypeStruct((local_sectors, rows, width), F32)
    offset, mine, theirs, ring = lax.optimization_barrier((offset, mine, theirs, ring))

    def partial_pieces(vector, loading):
        sent = apply_terms(targets, theirs, vector, left, right, loading, True)
        arrived = lax.ppermute(sent, CORE, [(0, 1), (1, 0)])
        kept = apply_terms(targets, mine, vector, left, right, loading, False)
        shape = (owners // 2, local_sectors, rows, width)
        own, *sent = pack(ring, mine, kept, arrived, shape)
        arrived = [along_ring(piece, step) for step, piece in enumerate(sent, 1)]
        return across_rings(meet(own, arrived))

    pieces = partial_pieces(wavefunction, True)
    devices = lax.axis_size(EVERY)
    sigma_first, again, sums = pl.pallas_call(
        first_kernel,
        out_shape=(row_shape, row_shape, jax.ShapeDtypeStruct((devices, 1, 128), F32)),
        in_specs=[SMEM, VMEM, VMEM, VMEM],
        out_specs=(VMEM, VMEM, VMEM),
        compiler_params=room(4),
        name="first",
    )(offset, pieces, wavefunction, preconditioner)
    sums = exchange(sums, EVERY)
    copies = pl.pallas_call(
        second_kernel,
        out_shape=jax.ShapeDtypeStruct((owners, local_sectors, rows, width), BF16),
        in_specs=[SMEM, VMEM, VMEM, VMEM, VMEM],
        out_specs=VMEM,
        compiler_params=room(4),
        name="second",
    )(offset, sums, again, wavefunction, preconditioner)
    pieces = partial_pieces(exchange(copies, OP), False)
    sigma_second = pl.pallas_call(
        sum_kernel,
        out_shape=row_shape,
        in_specs=[VMEM],
        out_specs=VMEM,
        compiler_params=room(4),
        name="last",
    )(pieces)
    return (sigma_first, sigma_second)


def solution(mesh):
    torus = Mesh(mesh.devices.reshape(2, 4, 4, 2, 2), EVERY)
    placed = (
        P(SECTOR, None, None),
        P(OP, SECTOR, None, None),
        P(OP, SECTOR, None, None),
        P(OP, SECTOR),
        P(SECTOR, OP, None),
    )
    return jax.shard_map(
        on_device,
        mesh=torus,
        in_specs=placed,
        out_specs=(P(SECTOR, OP, None), P(SECTOR, OP, None)),
        check_vma=False,
    )
```

```python
import functools
import itertools

import jax
import jax.numpy as jnp
from jax import lax
from jax.experimental import pallas as pl
from jax.experimental.pallas import tpu as pltpu
from jax.sharding import Mesh
from jax.sharding import PartitionSpec as P

SECTOR = ("sector_0", "sector_1")
OP = ("op_0", "op_1", "op_2")
EVERY = ("op_0", "op_1", "op_2", "sector_0", "sector_1")
CORE = "sector_1"
F32 = jnp.float32
BF16 = jnp.bfloat16
VMEM = pl.BlockSpec(memory_space=pltpu.VMEM)
SMEM = pl.BlockSpec(memory_space=pltpu.SMEM)
HBM = pl.BlockSpec(memory_space=pltpu.HBM)


def room(mebibytes):
    return pltpu.CompilerParams(vmem_limit_bytes=mebibytes * 2**20)


def exchange(pieces, axis):
    return lax.all_to_all(pieces, axis, split_axis=0, concat_axis=0, tiled=True)


def chosen_tasks(targets, core, order):
    local_sectors, terms = targets.shape

    def scan(task, count):
        target = targets[lax.rem(task, local_sectors), task // local_sectors]
        order[count] = task
        return count + (lax.rem(target // local_sectors, 2) == core[0]).astype(jnp.int32)

    return lax.fori_loop(0, local_sectors * terms, scan, jnp.int32(0))


def run_tasks(targets, order, count, source, lefts, rights, totals, touched, arrive):
    local_sectors = targets.shape[0]
    slots, width, _ = totals.shape
    for slot in range(slots):
        touched[slot] = 0

    def middle_of(task):
        vector = source(lax.rem(task, local_sectors))
        return jnp.dot(lefts[task], vector, preferred_element_type=F32).astype(BF16)

    def add(task, middle):
        target = targets[lax.rem(task, local_sectors), task // local_sectors]
        slot = target // (2 * local_sectors) * local_sectors + lax.rem(target, local_sectors)
        fresh = touched[slot] == 0
        touched[slot] = 1
        share = lax.dot_general(
            middle, rights[task], (((1,), (1,)), ((), ())), preferred_element_type=F32
        )
        totals[slot] = share + jnp.where(fresh, 0.0, totals[slot])

    def pair(index, carry):
        tasks = order[2 * index], order[2 * index + 1]
        for task in tasks:
            arrive(0, task)
        middles = [middle_of(task) for task in tasks]
        for task in tasks:
            arrive(1, task)
        for task, middle in zip(tasks, middles):
            add(task, middle)
        return carry

    lax.fori_loop(0, count // 2, pair, 0)

    @pl.when(lax.rem(count, 2) == 1)
    def _():
        task = order[count - 1]
        arrive(0, task)
        arrive(1, task)
        add(task, middle_of(task))

    for slot in range(slots):

        @pl.when(touched[slot] == 0)
        def _(slot=slot):
            totals[slot] = jnp.zeros((width, width), F32)


def apply_kernel(loading, sending, *refs):
    targets, core, vector, left, right, out, touched, order = refs[:8]
    rest = list(refs[8:])
    totals = rest.pop(0) if sending else out
    count = chosen_tasks(targets, core, order)
    if loading:
        lefts, rights, sems = rest

        def copy(side, task):
            source, buffer = ((left, lefts), (right, rights))[side]
            return pltpu.make_async_copy(source.at[task], buffer.at[task], sems.at[side, task])

        def start(sides, index, carry):
            for side in sides:
                copy(side, order[index]).start()
            return carry

        def arrive(side, task):
            copy(side, task).wait()

        early = jnp.minimum(count, 2)
        lax.fori_loop(0, early, functools.partial(start, (0,)), 0)
        lax.fori_loop(0, early, functools.partial(start, (1,)), 0)
        lax.fori_loop(early, count, functools.partial(start, (0, 1)), 0)
    else:
        lefts, rights = left, right

        def arrive(side, task):
            del side, task

    width = lefts.shape[1]

    def source(sector):
        if loading:
            return vector[sector]
        return vector[:, sector].reshape(width, width)

    run_tasks(targets, order, count, source, lefts, rights, totals, touched, arrive)
    if sending:
        out[...] = totals[...].astype(BF16)


def apply_terms(targets, core, vector, left, right, loading, sending):
    tasks, width, _ = left.shape
    slots = tasks // 2
    scratch = [pltpu.SMEM((slots,), jnp.int32), pltpu.SMEM((tasks + 1,), jnp.int32)]
    if sending:
        scratch += [pltpu.VMEM((slots, width, width), F32)]
    if loading:
        scratch += [
            pltpu.VMEM(left.shape, BF16),
            pltpu.VMEM(left.shape, BF16),
            pltpu.SemaphoreType.DMA((2, tasks)),
        ]
    return pl.pallas_call(
        functools.partial(apply_kernel, loading, sending),
        out_shape=jax.ShapeDtypeStruct((slots, width, width), BF16 if sending else F32),
        in_specs=[SMEM, SMEM, VMEM] + [HBM if loading else VMEM] * 2,
        out_specs=VMEM,
        scratch_shapes=scratch,
        compiler_params=room((50 if sending else 46) if loading else 8),
        cost_estimate=pl.CostEstimate(
            flops=2 * tasks * width**3, bytes_accessed=2 * tasks * width**2, transcendentals=0
        ),
        name=("load_" if loading else "") + ("send" if sending else "keep"),
    )(targets, core, vector, left, right)


def place(op_0, op_1, op_2, half, core):
    return (((op_0 * 4 + op_1) * 4 + op_2) * 2 + half) * 2 + core


def along_ring(value, step):
    pairs = []
    for op_0, op_1, op_2, half in itertools.product(range(2), range(4), range(4), range(2)):
        first, second = (op_1 + step) % 4, (op_2 + step) % 4
        pairs.append((place(op_0, op_1, op_2, half, 0), place(op_0, first, op_2, half, 0)))
        pairs.append((place(op_0, op_1, op_2, half, 1), place(op_0, op_1, second, half, 1)))
    return lax.ppermute(value, EVERY, pairs)


def across_rings(pieces):
    rest = list(itertools.product(range(2), range(4), range(2)))
    groups = [[place(low, ring, at, half, 0) for low, at, half in rest] for ring in range(4)]
    groups += [[place(low, at, ring, half, 1) for low, at, half in rest] for ring in range(4)]
    return lax.all_to_all(
        pieces, EVERY, split_axis=0, concat_axis=0, axis_index_groups=groups, tiled=True
    )


def pack_kernel(ring, core, kept, arrived, own, *sent):
    others, local_sectors, rows, _ = own.shape

    def one_block(index, carry):
        other, sector = index // local_sectors, lax.rem(index, local_sectors)
        low, at, half = other // 8, lax.rem(other // 2, 4), lax.rem(other, 2)
        slot = half * local_sectors + sector
        for step in range(4):
            to = lax.rem(ring[0] + step, 4)
            block = low * 16 + jnp.where(core[0] == 0, to * 4 + at, at * 4 + to)
            here = pl.ds(pl.multiple_of(block * rows, rows), rows)
            total = kept[slot, here, :] + arrived[slot, here, :].astype(F32)
            if step == 0:
                own[other, sector] = total
            else:
                sent[step - 1][other, sector] = total.astype(BF16)
        return carry

    lax.fori_loop(0, others * local_sectors, one_block, 0, unroll=8)


def pack(ring, core, kept, arrived, shape):
    return pl.pallas_call(
        pack_kernel,
        out_shape=[jax.ShapeDtypeStruct(shape, F32)] + [jax.ShapeDtypeStruct(shape, BF16)] * 3,
        in_specs=[SMEM, SMEM, VMEM, VMEM],
        out_specs=[VMEM] * 4,
        compiler_params=room(4),
        name="pack",
    )(ring, core, kept, arrived)


def meet_kernel(own, first, second, third, out):
    def one(index, carry):
        total = own[index] + first[index].astype(F32)
        total += second[index].astype(F32) + third[index].astype(F32)
        out[index] = total.astype(BF16)
        return carry

    lax.fori_loop(0, own.shape[0], one, 0, unroll=4)


def meet(own, arrived):
    return pl.pallas_call(
        meet_kernel,
        out_shape=jax.ShapeDtypeStruct(own.shape, BF16),
        in_specs=[VMEM] * 4,
        out_specs=VMEM,
        compiler_params=room(4),
        name="meet",
    )(own, *arrived)


def summed(pieces):
    shape = pieces.shape[1:]
    count = pieces.shape[0]

    def add(index, total):
        return total + pieces[index].astype(F32)

    return lax.fori_loop(0, count, add, jnp.zeros(shape, F32), unroll=8)


def lanes(value):
    local_sectors, rows, width = value.shape
    flat = jnp.sum(value.reshape(local_sectors * rows, width), axis=0, keepdims=True)
    return sum(flat[:, at : at + 128] for at in range(0, width, 128))


def first_kernel(offset, pieces, wave, precond, sigma, again, sums):
    rows = precond.shape[1]
    own = wave[:, pl.ds(pl.multiple_of(offset[0], rows), rows), :].astype(F32)
    total = summed(pieces)
    sigma[...] = total
    again[...] = total
    ratio, scaled = total / precond[...], own / precond[...]
    terms = (
        own * own,
        own * total,
        own * ratio,
        own * scaled,
        ratio * ratio,
        ratio * scaled,
        scaled * scaled,
    )
    one = jnp.concatenate([lanes(term) for term in terms] + [jnp.zeros((1, 128), F32)], axis=0)
    one = jnp.sum(one, axis=1, keepdims=True)
    row = lax.broadcasted_iota(jnp.int32, (8, 128), 0)
    lane = lax.broadcasted_iota(jnp.int32, (8, 128), 1)
    one = jnp.sum(jnp.where(row == lane, one, 0.0), axis=0, keepdims=True)
    sums[...] = jnp.broadcast_to(one[None], sums.shape)


def second_kernel(offset, sums, sigma, wave, precond, copies):
    rows = precond.shape[1]
    own = wave[:, pl.ds(pl.multiple_of(offset[0], rows), rows), :].astype(F32)
    whole = summed(sums)
    norm_sq, w_s, w_r, w_b, r_r, r_b, b_b = (whole[:, k : k + 1] for k in range(7))
    shift = w_s / norm_sq - 1.0
    projected = w_r - shift * w_b
    correction_sq = r_r - 2.0 * shift * r_b + shift * shift * b_b
    along = projected / norm_sq
    update_sq = correction_sq - projected * along
    scale = jnp.sqrt(norm_sq) * lax.rsqrt(update_sq + 1e-06)
    correction = (sigma[...] - shift[None] * own) / precond[...]
    new = ((correction - along[None] * own) * scale[None]).astype(BF16)
    copies[...] = jnp.broadcast_to(new[None], copies.shape)


def sum_kernel(pieces, sigma):
    sigma[...] = summed(pieces)


def on_device(wavefunction, left_blocks, right_blocks, target_sector, preconditioner):
    local_sectors, width, _ = wavefunction.shape
    rows = preconditioner.shape[1]
    owners = lax.axis_size(OP)
    offset = (lax.axis_index(OP) * rows).reshape(1)
    mine = lax.axis_index(CORE).reshape(1)
    theirs = 1 - mine
    ring = jnp.where(mine == 0, lax.axis_index("op_1"), lax.axis_index("op_2"))
    targets = target_sector.T
    left, right = (
        blocks.reshape(-1, width, width) for blocks in (left_blocks, right_blocks)
    )
    row_shape = jax.ShapeDtypeStruct((local_sectors, rows, width), F32)
    offset, mine, theirs, ring = lax.optimization_barrier((offset, mine, theirs, ring))

    def partial_pieces(vector, loading):
        sent = apply_terms(targets, theirs, vector, left, right, loading, True)
        arrived = lax.ppermute(sent, CORE, [(0, 1), (1, 0)])
        kept = apply_terms(targets, mine, vector, left, right, loading, False)
        shape = (owners // 2, local_sectors, rows, width)
        own, *sent = pack(ring, mine, kept, arrived, shape)
        arrived = [along_ring(sent[step - 1], step) for step in (2, 1, 3)]
        return across_rings(meet(own, arrived))

    pieces = partial_pieces(wavefunction, True)
    devices = lax.axis_size(EVERY)
    sigma_first, again, sums = pl.pallas_call(
        first_kernel,
        out_shape=(row_shape, row_shape, jax.ShapeDtypeStruct((devices, 1, 128), F32)),
        in_specs=[SMEM, VMEM, VMEM, VMEM],
        out_specs=(VMEM, VMEM, VMEM),
        compiler_params=room(4),
        name="first",
    )(offset, pieces, wavefunction, preconditioner)
    sums = exchange(sums, EVERY)
    copies = pl.pallas_call(
        second_kernel,
        out_shape=jax.ShapeDtypeStruct((owners, local_sectors, rows, width), BF16),
        in_specs=[SMEM, VMEM, VMEM, VMEM, VMEM],
        out_specs=VMEM,
        compiler_params=room(4),
        name="second",
    )(offset, sums, again, wavefunction, preconditioner)
    pieces = partial_pieces(exchange(copies, OP), False)
    sigma_second = pl.pallas_call(
        sum_kernel,
        out_shape=row_shape,
        in_specs=[VMEM],
        out_specs=VMEM,
        compiler_params=room(4),
        name="last",
    )(pieces)
    return (sigma_first, sigma_second)


def solution(mesh):
    torus = Mesh(mesh.devices.reshape(2, 4, 4, 2, 2), EVERY)
    placed = (
        P(SECTOR, None, None),
        P(OP, SECTOR, None, None),
        P(OP, SECTOR, None, None),
        P(OP, SECTOR),
        P(SECTOR, OP, None),
    )
    return jax.shard_map(
        on_device,
        mesh=torus,
        in_specs=placed,
        out_specs=(P(SECTOR, OP, None), P(SECTOR, OP, None)),
        check_vma=False,
    )
```

```python
import functools
import itertools

import jax
import jax.numpy as jnp
from jax import lax
from jax.experimental import pallas as pl
from jax.experimental.pallas import tpu as pltpu
from jax.sharding import Mesh
from jax.sharding import PartitionSpec as P

SECTOR = ("sector_0", "sector_1")
OP = ("op_0", "op_1", "op_2")
EVERY = ("op_0", "op_1", "op_2", "sector_0", "sector_1")
CORE = "sector_1"
F32 = jnp.float32
BF16 = jnp.bfloat16
VMEM = pl.BlockSpec(memory_space=pltpu.VMEM)
SMEM = pl.BlockSpec(memory_space=pltpu.SMEM)
HBM = pl.BlockSpec(memory_space=pltpu.HBM)


def room(mebibytes):
    return pltpu.CompilerParams(vmem_limit_bytes=mebibytes * 2**20)


def exchange(pieces, axis):
    return lax.all_to_all(pieces, axis, split_axis=0, concat_axis=0, tiled=True)


def chosen_tasks(targets, core, order, at):
    local_sectors, terms = targets.shape

    def scan(task, count):
        target = targets[lax.rem(task, local_sectors), task // local_sectors]
        order[count] = task
        return count + (lax.rem(target // local_sectors, 2) == core).astype(jnp.int32)

    return lax.fori_loop(0, local_sectors * terms, scan, jnp.int32(at))


def run_tasks(targets, order, count, source, lefts, rights, totals, touched, arrive):
    local_sectors = targets.shape[0]
    slots, width, _ = totals.shape
    for slot in range(slots):
        touched[slot] = 0

    def middle_of(task):
        vector = source(lax.rem(task, local_sectors))
        return jnp.dot(lefts[task], vector, preferred_element_type=F32).astype(BF16)

    def add(task, middle):
        target = targets[lax.rem(task, local_sectors), task // local_sectors]
        slot = target // (2 * local_sectors) * local_sectors + lax.rem(target, local_sectors)
        fresh = touched[slot] == 0
        touched[slot] = 1
        share = lax.dot_general(
            middle, rights[task], (((1,), (1,)), ((), ())), preferred_element_type=F32
        )
        totals[slot] = share + jnp.where(fresh, 0.0, totals[slot])

    def pair(index, carry):
        tasks = order[2 * index], order[2 * index + 1]
        for task in tasks:
            arrive(0, task)
        middles = [middle_of(task) for task in tasks]
        for task in tasks:
            arrive(1, task)
        for task, middle in zip(tasks, middles):
            add(task, middle)
        return carry

    lax.fori_loop(0, count // 2, pair, 0)

    @pl.when(lax.rem(count, 2) == 1)
    def _():
        task = order[count - 1]
        arrive(0, task)
        arrive(1, task)
        add(task, middle_of(task))

    for slot in range(slots):

        @pl.when(touched[slot] == 0)
        def _(slot=slot):
            totals[slot] = jnp.zeros((width, width), F32)


def send_first_kernel(
    targets, core, vector, left, right, out, lefts, rights, touched, order, totals, wave, sems, wave_sem
):
    tasks = left.shape[0]

    def copy(side, task):
        source, buffer = ((left, lefts), (right, rights))[side]
        return pltpu.make_async_copy(source.at[task], buffer.at[task], sems.at[side, task])

    def start(sides, index, carry):
        for side in sides:
            copy(side, order[index]).start()
        return carry

    def arrive(side, task):
        copy(side, task).wait()

    def rest(index, carry):
        for side in (0, 1):
            arrive(side, order[index])
        return carry

    whole = pltpu.make_async_copy(vector, wave, wave_sem)
    whole.start()
    count = chosen_tasks(targets, core[0], order, 0)
    chosen_tasks(targets, 1 - core[0], order, count)
    early = jnp.minimum(count, 2)
    lax.fori_loop(0, early, functools.partial(start, (0,)), 0)
    lax.fori_loop(0, early, functools.partial(start, (1,)), 0)
    lax.fori_loop(early, tasks, functools.partial(start, (0, 1)), 0)
    whole.wait()
    run_tasks(
        targets, order, count, lambda sector: wave[sector], lefts, rights, totals, touched, arrive
    )
    lax.fori_loop(count, tasks, rest, 0)
    out[...] = totals[...].astype(BF16)


def apply_kernel(sending, targets, core, vector, lefts, rights, out, touched, order, *totals):
    width = lefts.shape[1]
    count = chosen_tasks(targets, core[0], order, 0)

    def source(sector):
        return (vector[sector] if vector.shape[1] == width else vector[:, sector]).reshape(
            width, width
        )

    def arrive(side, task):
        del side, task

    total = totals[0] if sending else out
    run_tasks(targets, order, count, source, lefts, rights, total, touched, arrive)
    if sending:
        out[...] = total[...].astype(BF16)


def apply_terms(targets, core, vector, left, right, first, sending):
    tasks, width, _ = left.shape
    slots = tasks // 2
    scratch = [pltpu.SMEM((slots,), jnp.int32), pltpu.SMEM((tasks + 1,), jnp.int32)]
    if sending:
        scratch += [pltpu.VMEM((slots, width, width), F32)]
    out = jax.ShapeDtypeStruct((slots, width, width), BF16 if sending else F32)
    if first:
        scratch += [
            pltpu.VMEM(vector.shape, BF16),
            pltpu.SemaphoreType.DMA((2, tasks)),
            pltpu.SemaphoreType.DMA,
        ]
        vector, left, right = (
            pltpu.with_memory_space_constraint(value, pltpu.HBM) for value in (vector, left, right)
        )
        out = (out, jax.ShapeDtypeStruct(left.shape, BF16), jax.ShapeDtypeStruct(left.shape, BF16))
    return pl.pallas_call(
        send_first_kernel if first else functools.partial(apply_kernel, sending),
        out_shape=out,
        in_specs=[SMEM, SMEM] + [HBM if first else VMEM] * 3,
        out_specs=(VMEM, VMEM, VMEM) if first else VMEM,
        scratch_shapes=scratch,
        compiler_params=room(8 if first else 8),
        cost_estimate=pl.CostEstimate(
            flops=2 * tasks * width**3, bytes_accessed=2 * tasks * width**2, transcendentals=0
        ),
        name="send_first" if first else ("send" if sending else "keep"),
    )(targets, core, vector, left, right)


def place(op_0, op_1, op_2, half, core):
    return (((op_0 * 4 + op_1) * 4 + op_2) * 2 + half) * 2 + core


def along_ring(value, step):
    pairs = []
    for op_0, op_1, op_2, half in itertools.product(range(2), range(4), range(4), range(2)):
        first, second = (op_1 + step) % 4, (op_2 + step) % 4
        pairs.append((place(op_0, op_1, op_2, half, 0), place(op_0, first, op_2, half, 0)))
        pairs.append((place(op_0, op_1, op_2, half, 1), place(op_0, op_1, second, half, 1)))
    return lax.ppermute(value, EVERY, pairs)


def across_rings(pieces):
    rest = list(itertools.product(range(2), range(4), range(2)))
    groups = [[place(low, ring, at, half, 0) for low, at, half in rest] for ring in range(4)]
    groups += [[place(low, at, ring, half, 1) for low, at, half in rest] for ring in range(4)]
    return lax.all_to_all(
        pieces, EVERY, split_axis=0, concat_axis=0, axis_index_groups=groups, tiled=True
    )


def pack_kernel(ring, core, kept, arrived, own, *sent):
    others, local_sectors, rows, _ = own.shape

    def one_block(index, carry):
        other, sector = index // local_sectors, lax.rem(index, local_sectors)
        low, at, half = other // 8, lax.rem(other // 2, 4), lax.rem(other, 2)
        slot = half * local_sectors + sector
        for step in range(4):
            to = lax.rem(ring[0] + step, 4)
            block = low * 16 + jnp.where(core[0] == 0, to * 4 + at, at * 4 + to)
            here = pl.ds(pl.multiple_of(block * rows, rows), rows)
            total = kept[slot, here, :] + arrived[slot, here, :].astype(F32)
            if step == 0:
                own[other, sector] = total
            else:
                sent[step - 1][other, sector] = total.astype(BF16)
        return carry

    lax.fori_loop(0, others * local_sectors, one_block, 0, unroll=8)


def pack(ring, core, kept, arrived, shape):
    return pl.pallas_call(
        pack_kernel,
        out_shape=[jax.ShapeDtypeStruct(shape, F32)] + [jax.ShapeDtypeStruct(shape, BF16)] * 3,
        in_specs=[SMEM, SMEM, VMEM, VMEM],
        out_specs=[VMEM] * 4,
        compiler_params=room(4),
        name="pack",
    )(ring, core, kept, arrived)


def meet_kernel(own, first, second, third, out):
    def one(index, carry):
        total = own[index] + first[index].astype(F32)
        total += second[index].astype(F32) + third[index].astype(F32)
        out[index] = total.astype(BF16)
        return carry

    lax.fori_loop(0, own.shape[0], one, 0, unroll=4)


def meet(own, arrived):
    return pl.pallas_call(
        meet_kernel,
        out_shape=jax.ShapeDtypeStruct(own.shape, BF16),
        in_specs=[VMEM] * 4,
        out_specs=VMEM,
        compiler_params=room(4),
        name="meet",
    )(own, *arrived)


def summed(pieces):
    shape = pieces.shape[1:]
    count = pieces.shape[0]

    def add(index, total):
        return total + pieces[index].astype(F32)

    return lax.fori_loop(0, count, add, jnp.zeros(shape, F32), unroll=8)


def lanes(value):
    local_sectors, rows, width = value.shape
    flat = jnp.sum(value.reshape(local_sectors * rows, width), axis=0, keepdims=True)
    return sum(flat[:, at : at + 128] for at in range(0, width, 128))


def first_kernel(offset, pieces, wave, precond, sigma, again, sums):
    rows = precond.shape[1]
    own = wave[:, pl.ds(pl.multiple_of(offset[0], rows), rows), :].astype(F32)
    total = summed(pieces)
    sigma[...] = total
    again[...] = total
    ratio, scaled = total / precond[...], own / precond[...]
    terms = (
        own * own,
        own * total,
        own * ratio,
        own * scaled,
        ratio * ratio,
        ratio * scaled,
        scaled * scaled,
    )
    one = jnp.concatenate([lanes(term) for term in terms] + [jnp.zeros((1, 128), F32)], axis=0)
    one = jnp.sum(one, axis=1, keepdims=True)
    row = lax.broadcasted_iota(jnp.int32, (8, 128), 0)
    lane = lax.broadcasted_iota(jnp.int32, (8, 128), 1)
    one = jnp.sum(jnp.where(row == lane, one, 0.0), axis=0, keepdims=True)
    sums[...] = jnp.broadcast_to(one[None], sums.shape)


def second_kernel(offset, sums, sigma, wave, precond, copies):
    rows = precond.shape[1]
    own = wave[:, pl.ds(pl.multiple_of(offset[0], rows), rows), :].astype(F32)
    whole = summed(sums)
    norm_sq, w_s, w_r, w_b, r_r, r_b, b_b = (whole[:, k : k + 1] for k in range(7))
    shift = w_s / norm_sq - 1.0
    projected = w_r - shift * w_b
    correction_sq = r_r - 2.0 * shift * r_b + shift * shift * b_b
    along = projected / norm_sq
    update_sq = correction_sq - projected * along
    scale = jnp.sqrt(norm_sq) * lax.rsqrt(update_sq + 1e-06)
    correction = (sigma[...] - shift[None] * own) / precond[...]
    new = ((correction - along[None] * own) * scale[None]).astype(BF16)
    copies[...] = jnp.broadcast_to(new[None], copies.shape)


def sum_kernel(pieces, sigma):
    sigma[...] = summed(pieces)


def on_device(wavefunction, left_blocks, right_blocks, target_sector, preconditioner):
    local_sectors, width, _ = wavefunction.shape
    rows = preconditioner.shape[1]
    owners = lax.axis_size(OP)
    offset = (lax.axis_index(OP) * rows).reshape(1)
    mine = lax.axis_index(CORE).reshape(1)
    theirs = 1 - mine
    ring = jnp.where(mine == 0, lax.axis_index("op_1"), lax.axis_index("op_2"))
    targets = target_sector.T
    left, right = (
        blocks.reshape(-1, width, width) for blocks in (left_blocks, right_blocks)
    )
    row_shape = jax.ShapeDtypeStruct((local_sectors, rows, width), F32)
    offset, mine, theirs, ring = lax.optimization_barrier((offset, mine, theirs, ring))

    def partial_pieces(vector, left, right, first):
        sent = apply_terms(targets, theirs, vector, left, right, first, True)
        if first:
            sent, left, right = sent
        arrived = lax.ppermute(sent, CORE, [(0, 1), (1, 0)])
        kept = apply_terms(targets, mine, vector, left, right, False, False)
        shape = (owners // 2, local_sectors, rows, width)
        own, *sent = pack(ring, mine, kept, arrived, shape)
        arrived = [along_ring(sent[step - 1], step) for step in (2, 1, 3)]
        return across_rings(meet(own, arrived)), left, right

    pieces, left, right = partial_pieces(wavefunction, left, right, True)
    devices = lax.axis_size(EVERY)
    sigma_first, again, sums = pl.pallas_call(
        first_kernel,
        out_shape=(row_shape, row_shape, jax.ShapeDtypeStruct((devices, 1, 128), F32)),
        in_specs=[SMEM, VMEM, VMEM, VMEM],
        out_specs=(VMEM, VMEM, VMEM),
        compiler_params=room(4),
        name="first",
    )(offset, pieces, wavefunction, preconditioner)
    sums = exchange(sums, EVERY)
    copies = pl.pallas_call(
        second_kernel,
        out_shape=jax.ShapeDtypeStruct((owners, local_sectors, rows, width), BF16),
        in_specs=[SMEM, VMEM, VMEM, VMEM, VMEM],
        out_specs=VMEM,
        compiler_params=room(4),
        name="second",
    )(offset, sums, again, wavefunction, preconditioner)
    pieces, _, _ = partial_pieces(exchange(copies, OP), left, right, False)
    sigma_second = pl.pallas_call(
        sum_kernel,
        out_shape=row_shape,
        in_specs=[VMEM],
        out_specs=VMEM,
        compiler_params=room(4),
        name="last",
    )(pieces)
    return (sigma_first, sigma_second)


def solution(mesh):
    torus = Mesh(mesh.devices.reshape(2, 4, 4, 2, 2), EVERY)
    placed = (
        P(SECTOR, None, None),
        P(OP, SECTOR, None, None),
        P(OP, SECTOR, None, None),
        P(OP, SECTOR),
        P(SECTOR, OP, None),
    )
    return jax.shard_map(
        on_device,
        mesh=torus,
        in_specs=placed,
        out_specs=(P(SECTOR, OP, None), P(SECTOR, OP, None)),
        check_vma=False,
    )
```

```python
import functools
import itertools

import jax
import jax.numpy as jnp
from jax import lax
from jax.experimental import pallas as pl
from jax.experimental.pallas import tpu as pltpu
from jax.sharding import Mesh
from jax.sharding import PartitionSpec as P

SECTOR = ("sector_0", "sector_1")
OP = ("op_0", "op_1", "op_2")
EVERY = ("op_0", "op_1", "op_2", "sector_0", "sector_1")
CORE = "sector_1"
F32 = jnp.float32
BF16 = jnp.bfloat16
VMEM = pl.BlockSpec(memory_space=pltpu.VMEM)
SMEM = pl.BlockSpec(memory_space=pltpu.SMEM)
HBM = pl.BlockSpec(memory_space=pltpu.HBM)


def room(mebibytes):
    return pltpu.CompilerParams(vmem_limit_bytes=mebibytes * 2**20)


def exchange(pieces, axis):
    return lax.all_to_all(pieces, axis, split_axis=0, concat_axis=0, tiled=True)


def listed(targets, core, order, at):
    local_sectors, terms = targets.shape

    def scan(task, count):
        target = targets[lax.rem(task, local_sectors), task // local_sectors]
        order[count] = task
        return count + (lax.rem(target // local_sectors, 2) == core).astype(jnp.int32)

    return lax.fori_loop(0, local_sectors * terms, scan, at)


def slot_of(targets, task):
    local_sectors = targets.shape[0]
    target = targets[lax.rem(task, local_sectors), task // local_sectors]
    return target // (2 * local_sectors) * local_sectors + lax.rem(target, local_sectors)


def run_tasks(targets, order, begin, end, source, lefts, rights, totals, touched, arrive):
    local_sectors = targets.shape[0]

    def middle_of(task):
        vector = source(lax.rem(task, local_sectors))
        return jnp.dot(lefts[task], vector, preferred_element_type=F32).astype(BF16)

    def add(task, middle):
        slot = slot_of(targets, task)
        fresh = touched[slot] == 0
        touched[slot] = 1
        share = lax.dot_general(
            middle, rights[task], (((1,), (1,)), ((), ())), preferred_element_type=F32
        )
        totals[slot] = share + jnp.where(fresh, 0.0, totals[slot])

    def pair(index, carry):
        tasks = order[begin + 2 * index], order[begin + 2 * index + 1]
        for task in tasks:
            arrive(0, task)
        middles = [middle_of(task) for task in tasks]
        for task in tasks:
            arrive(1, task)
        for task, middle in zip(tasks, middles):
            add(task, middle)
        return carry

    lax.fori_loop(0, (end - begin) // 2, pair, 0)

    @pl.when(lax.rem(end - begin, 2) == 1)
    def _():
        task = order[end - 1]
        arrive(0, task)
        arrive(1, task)
        add(task, middle_of(task))


def clear(touched):
    for slot in range(touched.shape[0]):
        touched[slot] = 0


def fill(totals, touched):
    for slot in range(totals.shape[0]):

        @pl.when(touched[slot] == 0)
        def _(slot=slot):
            totals[slot] = jnp.zeros(totals.shape[1:], F32)


def early_kernel(first, targets, core, vector, left, right, out, kept, *refs):
    if first:
        lefts, rights, touched, order, totals, wave, sems, wave_sem = refs
    else:
        lefts, rights = left, right
        touched, order, totals = refs
    tasks, width, _ = lefts.shape

    def copy(side, task):
        origin, buffer = ((left, lefts), (right, rights))[side]
        return pltpu.make_async_copy(origin.at[task], buffer.at[task], sems.at[side, task])

    def start(sides, index, carry):
        for side in sides:
            copy(side, order[index]).start()
        return carry

    def arrive(side, task):
        if first:
            copy(side, task).wait()

    def rest(index, carry):
        for side in (0, 1):
            arrive(side, order[index])
        return carry

    def source(sector):
        return wave[sector] if first else vector[:, sector].reshape(width, width)

    if first:
        whole = pltpu.make_async_copy(vector, wave, wave_sem)
        whole.start()
    count = listed(targets, 1 - core[0], order, jnp.int32(0))
    listed(targets, core[0], order, count)
    if first:
        early = jnp.minimum(count, 2)
        lax.fori_loop(0, early, functools.partial(start, (0,)), 0)
        lax.fori_loop(0, early, functools.partial(start, (1,)), 0)
        lax.fori_loop(early, tasks, functools.partial(start, (0, 1)), 0)
        whole.wait()
    end = jnp.maximum(count, tasks // 2)
    clear(touched)
    run_tasks(targets, order, 0, count, source, lefts, rights, totals, touched, arrive)
    fill(totals, touched)
    out[...] = totals[...].astype(BF16)
    clear(touched)
    run_tasks(targets, order, count, end, source, lefts, rights, kept, touched, arrive)
    if first:
        lax.fori_loop(end, tasks, rest, 0)


def late_kernel(targets, core, vector, lefts, rights, begun, kept, touched, order):
    del begun
    tasks, width, _ = lefts.shape
    count = listed(targets, 1 - core[0], order, jnp.int32(0))
    listed(targets, core[0], order, count)
    end = jnp.maximum(count, tasks // 2)
    clear(touched)

    def mark(index, carry):
        touched[slot_of(targets, order[index])] = 1
        return carry

    def source(sector):
        return (vector[sector] if vector.shape[1] == width else vector[:, sector]).reshape(
            width, width
        )

    def arrive(side, task):
        del side, task

    lax.fori_loop(count, end, mark, 0)
    run_tasks(targets, order, end, tasks, source, lefts, rights, kept, touched, arrive)
    fill(kept, touched)


def apply_early(targets, core, vector, left, right, first):
    tasks, width, _ = left.shape
    slots = tasks // 2
    block = (slots, width, width)
    out = [jax.ShapeDtypeStruct(block, BF16), jax.ShapeDtypeStruct(block, F32)]
    scratch = [
        pltpu.SMEM((slots,), jnp.int32),
        pltpu.SMEM((tasks + 1,), jnp.int32),
        pltpu.VMEM(block, F32),
    ]
    if first:
        scratch += [
            pltpu.VMEM(vector.shape, BF16),
            pltpu.SemaphoreType.DMA((2, tasks)),
            pltpu.SemaphoreType.DMA,
        ]
        vector, left, right = (
            pltpu.with_memory_space_constraint(value, pltpu.HBM) for value in (vector, left, right)
        )
        out += [jax.ShapeDtypeStruct(left.shape, BF16)] * 2
    return pl.pallas_call(
        functools.partial(early_kernel, first),
        out_shape=out,
        in_specs=[SMEM, SMEM] + [HBM if first else VMEM] * 3,
        out_specs=[VMEM] * len(out),
        scratch_shapes=scratch,
        compiler_params=room(8),
        cost_estimate=work(tasks, width),
        name="early_first" if first else "early",
    )(targets, core, vector, left, right)


def apply_late(targets, core, vector, left, right, begun):
    tasks, width, _ = left.shape
    return pl.pallas_call(
        late_kernel,
        out_shape=jax.ShapeDtypeStruct(begun.shape, F32),
        in_specs=[SMEM, SMEM] + [VMEM] * 4,
        out_specs=VMEM,
        scratch_shapes=[
            pltpu.SMEM((tasks // 2,), jnp.int32),
            pltpu.SMEM((tasks + 1,), jnp.int32),
        ],
        input_output_aliases={5: 0},
        compiler_params=room(8),
        cost_estimate=work(tasks, width),
        name="late",
    )(targets, core, vector, left, right, begun)


def work(tasks, width):
    return pl.CostEstimate(
        flops=2 * tasks * width**3, bytes_accessed=2 * tasks * width**2, transcendentals=0
    )


def place(op_0, op_1, op_2, half, core):
    return (((op_0 * 4 + op_1) * 4 + op_2) * 2 + half) * 2 + core


def along_ring(value, step):
    pairs = []
    for op_0, op_1, op_2, half in itertools.product(range(2), range(4), range(4), range(2)):
        first, second = (op_1 + step) % 4, (op_2 + step) % 4
        pairs.append((place(op_0, op_1, op_2, half, 0), place(op_0, first, op_2, half, 0)))
        pairs.append((place(op_0, op_1, op_2, half, 1), place(op_0, op_1, second, half, 1)))
    return lax.ppermute(value, EVERY, pairs)


def across_rings(pieces):
    rest = list(itertools.product(range(2), range(4), range(2)))
    groups = [[place(low, ring, at, half, 0) for low, at, half in rest] for ring in range(4)]
    groups += [[place(low, at, ring, half, 1) for low, at, half in rest] for ring in range(4)]
    return lax.all_to_all(
        pieces, EVERY, split_axis=0, concat_axis=0, axis_index_groups=groups, tiled=True
    )


def pack_kernel(ring, core, kept, arrived, own, *sent):
    others, local_sectors, rows, _ = own.shape
    near, far = rows, 4 * rows
    ring_stride = jnp.where(core[0] == 0, far, near)
    at_stride = jnp.where(core[0] == 0, near, far)
    to = [lax.rem(ring[0] + step, 4) * ring_stride for step in range(4)]

    def one_place(place, carry):
        base = place // 4 * (16 * rows) + lax.rem(place, 4) * at_stride
        for step, half, sector in itertools.product(range(4), range(2), range(local_sectors)):
            here = pl.ds(pl.multiple_of(base + to[step], rows), rows)
            slot = half * local_sectors + sector
            total = kept[slot, here, :] + arrived[slot, here, :].astype(F32)
            if step == 0:
                own[2 * place + half, sector] = total
            else:
                sent[step - 1][2 * place + half, sector] = total.astype(BF16)
        return carry

    lax.fori_loop(0, others // 2, one_place, 0)


def pack(ring, core, kept, arrived, shape):
    return pl.pallas_call(
        pack_kernel,
        out_shape=[jax.ShapeDtypeStruct(shape, F32)] + [jax.ShapeDtypeStruct(shape, BF16)] * 3,
        in_specs=[SMEM, SMEM, VMEM, VMEM],
        out_specs=[VMEM] * 4,
        compiler_params=room(4),
        name="pack",
    )(ring, core, kept, arrived)


def meet_kernel(own, first, second, third, out):
    def one(index, carry):
        total = own[index] + first[index].astype(F32)
        total += second[index].astype(F32) + third[index].astype(F32)
        out[index] = total.astype(BF16)
        return carry

    lax.fori_loop(0, own.shape[0], one, 0, unroll=4)


def meet(own, arrived):
    return pl.pallas_call(
        meet_kernel,
        out_shape=jax.ShapeDtypeStruct(own.shape, BF16),
        in_specs=[VMEM] * 4,
        out_specs=VMEM,
        compiler_params=room(4),
        name="meet",
    )(own, *arrived)


def summed(pieces):
    shape = pieces.shape[1:]
    count = pieces.shape[0]

    def add(index, total):
        return total + pieces[index].astype(F32)

    return lax.fori_loop(0, count, add, jnp.zeros(shape, F32), unroll=8)


def lanes(value):
    local_sectors, rows, width = value.shape
    flat = jnp.sum(value.reshape(local_sectors * rows, width), axis=0, keepdims=True)
    return sum(flat[:, at : at + 128] for at in range(0, width, 128))


def first_kernel(offset, pieces, wave, precond, sigma, again, sums):
    rows = precond.shape[1]
    own = wave[:, pl.ds(pl.multiple_of(offset[0], rows), rows), :].astype(F32)
    total = summed(pieces)
    sigma[...] = total
    again[...] = total
    ratio, scaled = total / precond[...], own / precond[...]
    terms = (
        own * own,
        own * total,
        own * ratio,
        own * scaled,
        ratio * ratio,
        ratio * scaled,
        scaled * scaled,
    )
    one = jnp.concatenate([lanes(term) for term in terms] + [jnp.zeros((1, 128), F32)], axis=0)
    one = jnp.sum(one, axis=1, keepdims=True)
    row = lax.broadcasted_iota(jnp.int32, (8, 128), 0)
    lane = lax.broadcasted_iota(jnp.int32, (8, 128), 1)
    one = jnp.sum(jnp.where(row == lane, one, 0.0), axis=0, keepdims=True)
    sums[...] = jnp.broadcast_to(one[None], sums.shape)


def second_kernel(offset, sums, sigma, wave, precond, copies):
    rows = precond.shape[1]
    own = wave[:, pl.ds(pl.multiple_of(offset[0], rows), rows), :].astype(F32)
    whole = summed(sums)
    norm_sq, w_s, w_r, w_b, r_r, r_b, b_b = (whole[:, k : k + 1] for k in range(7))
    shift = w_s / norm_sq - 1.0
    projected = w_r - shift * w_b
    correction_sq = r_r - 2.0 * shift * r_b + shift * shift * b_b
    along = projected / norm_sq
    update_sq = correction_sq - projected * along
    scale = jnp.sqrt(norm_sq) * lax.rsqrt(update_sq + 1e-06)
    correction = (sigma[...] - shift[None] * own) / precond[...]
    new = ((correction - along[None] * own) * scale[None]).astype(BF16)
    copies[...] = jnp.broadcast_to(new[None], copies.shape)


def sum_kernel(pieces, sigma):
    sigma[...] = summed(pieces)


def on_device(wavefunction, left_blocks, right_blocks, target_sector, preconditioner):
    local_sectors, width, _ = wavefunction.shape
    rows = preconditioner.shape[1]
    owners = lax.axis_size(OP)
    offset = (lax.axis_index(OP) * rows).reshape(1)
    mine = lax.axis_index(CORE).reshape(1)
    ring = jnp.where(mine == 0, lax.axis_index("op_1"), lax.axis_index("op_2"))
    targets = target_sector.T
    left, right = (
        blocks.reshape(-1, width, width) for blocks in (left_blocks, right_blocks)
    )
    row_shape = jax.ShapeDtypeStruct((local_sectors, rows, width), F32)
    offset, mine, ring = lax.optimization_barrier((offset, mine, ring))

    def partial_pieces(vector, left, right, first):
        sent, begun, *blocks = apply_early(targets, mine, vector, left, right, first)
        left, right = blocks if first else (left, right)
        arrived = lax.ppermute(sent, CORE, [(0, 1), (1, 0)])
        kept = apply_late(targets, mine, vector, left, right, begun)
        shape = (owners // 2, local_sectors, rows, width)
        own, *sent = pack(ring, mine, kept, arrived, shape)
        arrived = [along_ring(sent[step - 1], step) for step in (2, 1, 3)]
        return across_rings(meet(own, arrived)), left, right

    pieces, left, right = partial_pieces(wavefunction, left, right, True)
    devices = lax.axis_size(EVERY)
    sigma_first, again, sums = pl.pallas_call(
        first_kernel,
        out_shape=(row_shape, row_shape, jax.ShapeDtypeStruct((devices, 1, 128), F32)),
        in_specs=[SMEM, VMEM, VMEM, VMEM],
        out_specs=(VMEM, VMEM, VMEM),
        compiler_params=room(4),
        name="first",
    )(offset, pieces, wavefunction, preconditioner)
    sums = exchange(sums, EVERY)
    copies = pl.pallas_call(
        second_kernel,
        out_shape=jax.ShapeDtypeStruct((owners, local_sectors, rows, width), BF16),
        in_specs=[SMEM, VMEM, VMEM, VMEM, VMEM],
        out_specs=VMEM,
        compiler_params=room(4),
        name="second",
    )(offset, sums, again, wavefunction, preconditioner)
    pieces, _, _ = partial_pieces(exchange(copies, OP), left, right, False)
    sigma_second = pl.pallas_call(
        sum_kernel,
        out_shape=row_shape,
        in_specs=[VMEM],
        out_specs=VMEM,
        compiler_params=room(4),
        name="last",
    )(pieces)
    return (sigma_first, sigma_second)


def solution(mesh):
    torus = Mesh(mesh.devices.reshape(2, 4, 4, 2, 2), EVERY)
    placed = (
        P(SECTOR, None, None),
        P(OP, SECTOR, None, None),
        P(OP, SECTOR, None, None),
        P(OP, SECTOR),
        P(SECTOR, OP, None),
    )
    return jax.shard_map(
        on_device,
        mesh=torus,
        in_specs=placed,
        out_specs=(P(SECTOR, OP, None), P(SECTOR, OP, None)),
        check_vma=False,
    )
```

```python
import functools
import itertools
import random

import jax
import jax.numpy as jnp
from jax import lax
from jax.experimental import pallas as pl
from jax.experimental.pallas import tpu as pltpu
from jax.sharding import Mesh
from jax.sharding import PartitionSpec as P

SECTOR = ("sector_0", "sector_1")
OP = ("op_0", "op_1", "op_2")
EVERY = ("op_0", "op_1", "op_2", "sector_0", "sector_1")
CORE = "sector_1"
F32 = jnp.float32
BF16 = jnp.bfloat16
VMEM = pl.BlockSpec(memory_space=pltpu.VMEM)
SMEM = pl.BlockSpec(memory_space=pltpu.SMEM)
HBM = pl.BlockSpec(memory_space=pltpu.HBM)


def room(mebibytes):
    return pltpu.CompilerParams(vmem_limit_bytes=mebibytes * 2**20)


def place(op_0, op_1, op_2, half, core):
    return (((op_0 * 4 + op_1) * 4 + op_2) * 2 + half) * 2 + core


def mixed(members, seed):
    members = list(members)
    random.Random(seed).shuffle(members)
    return members


OP_ORDER = mixed(itertools.product(range(2), range(4), range(4)), 8)
REST_ORDER = mixed(itertools.product(range(2), range(4), range(2)), 3)
OP_AT = [(low * 4 + first) * 4 + second for low, first, second in OP_ORDER]
REST_AT = [(low * 4 + at) * 2 + half for low, at, half in REST_ORDER]


def exchange(pieces, groups):
    return lax.all_to_all(
        pieces, EVERY, split_axis=0, concat_axis=0, axis_index_groups=groups, tiled=True
    )


def with_everyone(pieces):
    return exchange(pieces, [mixed(range(lax.axis_size(EVERY)), 0)])


def over_terms(pieces):
    sectors = itertools.product(range(2), range(2))
    return exchange(
        pieces, [[place(*op, half, core) for op in OP_ORDER] for half, core in sectors]
    )


def listed(targets, core, order, at):
    local_sectors, terms = targets.shape

    def scan(task, count):
        target = targets[lax.rem(task, local_sectors), task // local_sectors]
        order[count] = task
        return count + (lax.rem(target // local_sectors, 2) == core).astype(jnp.int32)

    return lax.fori_loop(0, local_sectors * terms, scan, at)


def slot_of(targets, task):
    local_sectors = targets.shape[0]
    target = targets[lax.rem(task, local_sectors), task // local_sectors]
    return target // (2 * local_sectors) * local_sectors + lax.rem(target, local_sectors)


def run_tasks(targets, order, begin, end, source, lefts, rights, totals, touched, arrive):
    local_sectors = targets.shape[0]

    def middle_of(task):
        vector = source(lax.rem(task, local_sectors))
        return jnp.dot(lefts[task], vector, preferred_element_type=F32).astype(BF16)

    def add(task, middle):
        slot = slot_of(targets, task)
        fresh = touched[slot] == 0
        touched[slot] = 1
        share = lax.dot_general(
            middle, rights[task], (((1,), (1,)), ((), ())), preferred_element_type=F32
        )
        totals[slot] = share + jnp.where(fresh, 0.0, totals[slot])

    def pair(index, carry):
        tasks = order[begin + 2 * index], order[begin + 2 * index + 1]
        for task in tasks:
            arrive(0, task)
        middles = [middle_of(task) for task in tasks]
        for task in tasks:
            arrive(1, task)
        for task, middle in zip(tasks, middles):
            add(task, middle)
        return carry

    lax.fori_loop(0, (end - begin) // 2, pair, 0)

    @pl.when(lax.rem(end - begin, 2) == 1)
    def _():
        task = order[end - 1]
        arrive(0, task)
        arrive(1, task)
        add(task, middle_of(task))


def clear(touched):
    for slot in range(touched.shape[0]):
        touched[slot] = 0


def fill(totals, touched):
    for slot in range(totals.shape[0]):

        @pl.when(touched[slot] == 0)
        def _(slot=slot):
            totals[slot] = jnp.zeros(totals.shape[1:], F32)


def early_kernel(first, targets, core, vector, left, right, out, kept, *refs):
    if first:
        lefts, rights, touched, order, totals, wave, sems, wave_sem = refs
    else:
        lefts, rights = left, right
        wave, touched, order, totals = refs
        rows = vector.shape[2]
        for index, owner in enumerate(OP_AT):
            wave[:, owner * rows : (owner + 1) * rows, :] = vector[index]
    tasks = lefts.shape[0]

    def copy(side, task):
        origin, buffer = ((left, lefts), (right, rights))[side]
        return pltpu.make_async_copy(origin.at[task], buffer.at[task], sems.at[side, task])

    def start(sides, index, carry):
        for side in sides:
            copy(side, order[index]).start()
        return carry

    def arrive(side, task):
        if first:
            copy(side, task).wait()

    def rest(index, carry):
        for side in (0, 1):
            arrive(side, order[index])
        return carry

    def source(sector):
        return wave[sector]

    if first:
        whole = pltpu.make_async_copy(vector, wave, wave_sem)
        whole.start()
    count = listed(targets, 1 - core[0], order, jnp.int32(0))
    listed(targets, core[0], order, count)
    if first:
        early = jnp.minimum(count, 2)
        lax.fori_loop(0, early, functools.partial(start, (0,)), 0)
        lax.fori_loop(0, early, functools.partial(start, (1,)), 0)
        lax.fori_loop(early, tasks, functools.partial(start, (0, 1)), 0)
        whole.wait()
    end = jnp.maximum(count, tasks // 2)
    clear(touched)
    run_tasks(targets, order, 0, count, source, lefts, rights, totals, touched, arrive)
    fill(totals, touched)
    out[...] = totals[...].astype(BF16)
    clear(touched)
    run_tasks(targets, order, count, end, source, lefts, rights, kept, touched, arrive)
    if first:
        lax.fori_loop(end, tasks, rest, 0)


def late_kernel(targets, core, vector, lefts, rights, begun, kept, touched, order):
    del begun
    tasks = lefts.shape[0]
    count = listed(targets, 1 - core[0], order, jnp.int32(0))
    listed(targets, core[0], order, count)
    end = jnp.maximum(count, tasks // 2)
    clear(touched)

    def mark(index, carry):
        touched[slot_of(targets, order[index])] = 1
        return carry

    def source(sector):
        return vector[sector]

    def arrive(side, task):
        del side, task

    lax.fori_loop(count, end, mark, 0)
    run_tasks(targets, order, end, tasks, source, lefts, rights, kept, touched, arrive)
    fill(kept, touched)


def apply_early(targets, core, vector, left, right, first):
    tasks, width, _ = left.shape
    slots = tasks // 2
    block = (slots, width, width)
    out = [jax.ShapeDtypeStruct(block, BF16), jax.ShapeDtypeStruct(block, F32)]
    scratch = [
        pltpu.SMEM((slots,), jnp.int32),
        pltpu.SMEM((tasks + 1,), jnp.int32),
        pltpu.VMEM(block, F32),
    ]
    if first:
        scratch += [
            pltpu.VMEM(vector.shape, BF16),
            pltpu.SemaphoreType.DMA((2, tasks)),
            pltpu.SemaphoreType.DMA,
        ]
        vector, left, right = (
            pltpu.with_memory_space_constraint(value, pltpu.HBM) for value in (vector, left, right)
        )
        out += [jax.ShapeDtypeStruct(left.shape, BF16)] * 2
    else:
        out += [jax.ShapeDtypeStruct((vector.shape[1], width, width), BF16)]
    return pl.pallas_call(
        functools.partial(early_kernel, first),
        out_shape=out,
        in_specs=[SMEM, SMEM] + [HBM if first else VMEM] * 3,
        out_specs=[VMEM] * len(out),
        scratch_shapes=scratch,
        compiler_params=room(8),
        cost_estimate=work(tasks, width),
        name="early_first" if first else "early",
    )(targets, core, vector, left, right)


def apply_late(targets, core, vector, left, right, begun):
    tasks, width, _ = left.shape
    return pl.pallas_call(
        late_kernel,
        out_shape=jax.ShapeDtypeStruct(begun.shape, F32),
        in_specs=[SMEM, SMEM] + [VMEM] * 4,
        out_specs=VMEM,
        scratch_shapes=[
            pltpu.SMEM((tasks // 2,), jnp.int32),
            pltpu.SMEM((tasks + 1,), jnp.int32),
        ],
        input_output_aliases={5: 0},
        compiler_params=room(8),
        cost_estimate=work(tasks, width),
        name="late",
    )(targets, core, vector, left, right, begun)


def work(tasks, width):
    return pl.CostEstimate(
        flops=2 * tasks * width**3, bytes_accessed=2 * tasks * width**2, transcendentals=0
    )


def along_ring(value, step):
    pairs = []
    for op_0, op_1, op_2, half in itertools.product(range(2), range(4), range(4), range(2)):
        first, second = (op_1 + step) % 4, (op_2 + step) % 4
        pairs.append((place(op_0, op_1, op_2, half, 0), place(op_0, first, op_2, half, 0)))
        pairs.append((place(op_0, op_1, op_2, half, 1), place(op_0, op_1, second, half, 1)))
    return lax.ppermute(value, EVERY, pairs)


def across_rings(pieces):
    rest = REST_ORDER
    groups = [[place(low, ring, at, half, 0) for low, at, half in rest] for ring in range(4)]
    groups += [[place(low, at, ring, half, 1) for low, at, half in rest] for ring in range(4)]
    return exchange(pieces, groups)


def pack_kernel(ring, core, kept, arrived, own, *sent):
    others, local_sectors, rows, _ = own.shape
    near, far = rows, 4 * rows
    ring_stride = jnp.where(core[0] == 0, far, near)
    at_stride = jnp.where(core[0] == 0, near, far)
    to = [lax.rem(ring[0] + step, 4) * ring_stride for step in range(4)]

    def one_place(place, carry):
        base = place // 4 * (16 * rows) + lax.rem(place, 4) * at_stride
        for step, half, sector in itertools.product(range(4), range(2), range(local_sectors)):
            here = pl.ds(pl.multiple_of(base + to[step], rows), rows)
            slot = half * local_sectors + sector
            total = kept[slot, here, :] + arrived[slot, here, :].astype(F32)
            if step == 0:
                own[2 * place + half, sector] = total
            else:
                sent[step - 1][2 * place + half, sector] = total.astype(BF16)
        return carry

    lax.fori_loop(0, others // 2, one_place, 0)


def pack(ring, core, kept, arrived, shape):
    return pl.pallas_call(
        pack_kernel,
        out_shape=[jax.ShapeDtypeStruct(shape, F32)] + [jax.ShapeDtypeStruct(shape, BF16)] * 3,
        in_specs=[SMEM, SMEM, VMEM, VMEM],
        out_specs=[VMEM] * 4,
        compiler_params=room(4),
        name="pack",
    )(ring, core, kept, arrived)


def meet_kernel(own, first, second, third, out):
    for to, index in enumerate(REST_AT):
        total = own[index] + first[index].astype(F32)
        total += second[index].astype(F32) + third[index].astype(F32)
        out[to] = total.astype(BF16)


def meet(own, arrived):
    return pl.pallas_call(
        meet_kernel,
        out_shape=jax.ShapeDtypeStruct(own.shape, BF16),
        in_specs=[VMEM] * 4,
        out_specs=VMEM,
        compiler_params=room(4),
        name="meet",
    )(own, *arrived)


def summed(pieces):
    shape = pieces.shape[1:]
    count = pieces.shape[0]

    def add(index, total):
        return total + pieces[index].astype(F32)

    return lax.fori_loop(0, count, add, jnp.zeros(shape, F32), unroll=8)


def lanes(value):
    local_sectors, rows, width = value.shape
    flat = jnp.sum(value.reshape(local_sectors * rows, width), axis=0, keepdims=True)
    return sum(flat[:, at : at + 128] for at in range(0, width, 128))


def first_kernel(offset, pieces, wave, precond, sigma, again, sums):
    rows = precond.shape[1]
    own = wave[:, pl.ds(pl.multiple_of(offset[0], rows), rows), :].astype(F32)
    total = summed(pieces)
    sigma[...] = total
    again[...] = total
    ratio, scaled = total / precond[...], own / precond[...]
    terms = (
        own * own,
        own * total,
        own * ratio,
        own * scaled,
        ratio * ratio,
        ratio * scaled,
        scaled * scaled,
    )
    one = jnp.concatenate([lanes(term) for term in terms] + [jnp.zeros((1, 128), F32)], axis=0)
    one = jnp.sum(one, axis=1, keepdims=True)
    row = lax.broadcasted_iota(jnp.int32, (8, 128), 0)
    lane = lax.broadcasted_iota(jnp.int32, (8, 128), 1)
    one = jnp.sum(jnp.where(row == lane, one, 0.0), axis=0, keepdims=True)
    sums[...] = jnp.broadcast_to(one[None], sums.shape)


def second_kernel(offset, sums, sigma, wave, precond, copies):
    rows = precond.shape[1]
    own = wave[:, pl.ds(pl.multiple_of(offset[0], rows), rows), :].astype(F32)
    whole = summed(sums)
    norm_sq, w_s, w_r, w_b, r_r, r_b, b_b = (whole[:, k : k + 1] for k in range(7))
    shift = w_s / norm_sq - 1.0
    projected = w_r - shift * w_b
    correction_sq = r_r - 2.0 * shift * r_b + shift * shift * b_b
    along = projected / norm_sq
    update_sq = correction_sq - projected * along
    scale = jnp.sqrt(norm_sq) * lax.rsqrt(update_sq + 1e-06)
    correction = (sigma[...] - shift[None] * own) / precond[...]
    new = ((correction - along[None] * own) * scale[None]).astype(BF16)
    copies[...] = jnp.broadcast_to(new[None], copies.shape)


def sum_kernel(pieces, sigma):
    sigma[...] = summed(pieces)


def on_device(wavefunction, left_blocks, right_blocks, target_sector, preconditioner):
    local_sectors, width, _ = wavefunction.shape
    rows = preconditioner.shape[1]
    owners = lax.axis_size(OP)
    offset = (lax.axis_index(OP) * rows).reshape(1)
    mine = lax.axis_index(CORE).reshape(1)
    ring = jnp.where(mine == 0, lax.axis_index("op_1"), lax.axis_index("op_2"))
    targets = target_sector.T
    left, right = (
        blocks.reshape(-1, width, width) for blocks in (left_blocks, right_blocks)
    )
    row_shape = jax.ShapeDtypeStruct((local_sectors, rows, width), F32)
    offset, mine, ring = lax.optimization_barrier((offset, mine, ring))

    def partial_pieces(vector, left, right, first):
        sent, begun, *rest = apply_early(targets, mine, vector, left, right, first)
        if first:
            left, right = rest
        else:
            (vector,) = rest
        arrived = lax.ppermute(sent, CORE, [(0, 1), (1, 0)])
        kept = apply_late(targets, mine, vector, left, right, begun)
        shape = (owners // 2, local_sectors, rows, width)
        own, *sent = pack(ring, mine, kept, arrived, shape)
        arrived = [along_ring(sent[step - 1], step) for step in (2, 1, 3)]
        return across_rings(meet(own, arrived)), left, right

    pieces, left, right = partial_pieces(wavefunction, left, right, True)
    devices = lax.axis_size(EVERY)
    sigma_first, again, sums = pl.pallas_call(
        first_kernel,
        out_shape=(row_shape, row_shape, jax.ShapeDtypeStruct((devices, 1, 128), F32)),
        in_specs=[SMEM, VMEM, VMEM, VMEM],
        out_specs=(VMEM, VMEM, VMEM),
        compiler_params=room(4),
        name="first",
    )(offset, pieces, wavefunction, preconditioner)
    sums = with_everyone(sums)
    copies = pl.pallas_call(
        second_kernel,
        out_shape=jax.ShapeDtypeStruct((owners, local_sectors, rows, width), BF16),
        in_specs=[SMEM, VMEM, VMEM, VMEM, VMEM],
        out_specs=VMEM,
        compiler_params=room(4),
        name="second",
    )(offset, sums, again, wavefunction, preconditioner)
    pieces, _, _ = partial_pieces(over_terms(copies), left, right, False)
    sigma_second = pl.pallas_call(
        sum_kernel,
        out_shape=row_shape,
        in_specs=[VMEM],
        out_specs=VMEM,
        compiler_params=room(4),
        name="last",
    )(pieces)
    return (sigma_first, sigma_second)


def solution(mesh):
    torus = Mesh(mesh.devices.reshape(2, 4, 4, 2, 2), EVERY)
    placed = (
        P(SECTOR, None, None),
        P(OP, SECTOR, None, None),
        P(OP, SECTOR, None, None),
        P(OP, SECTOR),
        P(SECTOR, OP, None),
    )
    return jax.shard_map(
        on_device,
        mesh=torus,
        in_specs=placed,
        out_specs=(P(SECTOR, OP, None), P(SECTOR, OP, None)),
        check_vma=False,
    )
```

```python
import functools
import itertools
import random

import jax
import jax.numpy as jnp
from jax import lax
from jax.experimental import pallas as pl
from jax.experimental.pallas import tpu as pltpu
from jax.sharding import Mesh
from jax.sharding import PartitionSpec as P

SECTOR = ("sector_0", "sector_1")
OP = ("op_0", "op_1", "op_2")
EVERY = ("op_0", "op_1", "op_2", "sector_0", "sector_1")
CORE = "sector_1"
F32 = jnp.float32
BF16 = jnp.bfloat16
VMEM = pl.BlockSpec(memory_space=pltpu.VMEM)
SMEM = pl.BlockSpec(memory_space=pltpu.SMEM)
HBM = pl.BlockSpec(memory_space=pltpu.HBM)


def room(mebibytes):
    return pltpu.CompilerParams(vmem_limit_bytes=mebibytes * 2**20)


def place(op_0, op_1, op_2, half, core):
    return (((op_0 * 4 + op_1) * 4 + op_2) * 2 + half) * 2 + core


def mixed(members, seed):
    members = list(members)
    random.Random(seed).shuffle(members)
    return members


OP_ORDER = mixed(itertools.product(range(2), range(4), range(4)), 8)
REST_ORDER = mixed(itertools.product(range(2), range(4), range(2)), 3)
OP_AT = [(low * 4 + first) * 4 + second for low, first, second in OP_ORDER]
REST_AT = [(low * 4 + at) * 2 + half for low, at, half in REST_ORDER]


def exchange(pieces, groups):
    return lax.all_to_all(
        pieces, EVERY, split_axis=0, concat_axis=0, axis_index_groups=groups, tiled=True
    )


def with_everyone(pieces):
    return exchange(pieces, [mixed(range(lax.axis_size(EVERY)), 0)])


def over_terms(pieces):
    sectors = itertools.product(range(2), range(2))
    return exchange(
        pieces, [[place(*op, half, core) for op in OP_ORDER] for half, core in sectors]
    )


def listed(targets, core, order, at):
    local_sectors, terms = targets.shape

    def scan(task, count):
        target = targets[lax.rem(task, local_sectors), task // local_sectors]
        order[count] = task
        return count + (lax.rem(target // local_sectors, 2) == core).astype(jnp.int32)

    return lax.fori_loop(0, local_sectors * terms, scan, at)


def slot_of(targets, task):
    local_sectors = targets.shape[0]
    target = targets[lax.rem(task, local_sectors), task // local_sectors]
    return target // (2 * local_sectors) * local_sectors + lax.rem(target, local_sectors)


def run_tasks(targets, order, begin, end, source, lefts, rights, totals, touched, arrive):
    local_sectors = targets.shape[0]

    def middle_of(task):
        vector = source(lax.rem(task, local_sectors))
        return jnp.dot(lefts[task], vector, preferred_element_type=F32).astype(BF16)

    def add(task, middle):
        slot = slot_of(targets, task)
        fresh = touched[slot] == 0
        touched[slot] = 1
        share = lax.dot_general(
            middle, rights[task], (((1,), (1,)), ((), ())), preferred_element_type=F32
        )
        totals[slot] = share + jnp.where(fresh, 0.0, totals[slot])

    def pair(index, carry):
        tasks = order[begin + 2 * index], order[begin + 2 * index + 1]
        for task in tasks:
            arrive(0, task)
        middles = [middle_of(task) for task in tasks]
        for task in tasks:
            arrive(1, task)
        for task, middle in zip(tasks, middles):
            add(task, middle)
        return carry

    lax.fori_loop(0, (end - begin) // 2, pair, 0)

    @pl.when(lax.rem(end - begin, 2) == 1)
    def _():
        task = order[end - 1]
        arrive(0, task)
        arrive(1, task)
        add(task, middle_of(task))


def clear(touched):
    for slot in range(touched.shape[0]):
        touched[slot] = 0


def fill(totals, touched):
    for slot in range(totals.shape[0]):

        @pl.when(touched[slot] == 0)
        def _(slot=slot):
            totals[slot] = jnp.zeros(totals.shape[1:], F32)


def early_kernel(first, targets, core, vector, left, right, out, kept, *refs):
    if first:
        lefts, rights, touched, order, totals, wave, known, sems, wave_sem, known_sem = refs
        whole = pltpu.make_async_copy(vector, wave, wave_sem)
        listing = pltpu.make_async_copy(targets, known, known_sem)
        listing.start()
        whole.start()
        listing.wait()
        targets = known
    else:
        lefts, rights = left, right
        wave, touched, order, totals = refs
        rows = vector.shape[2]
        for index, owner in enumerate(OP_AT):
            wave[:, owner * rows : (owner + 1) * rows, :] = vector[index]
    tasks = lefts.shape[0]

    def copy(side, task):
        origin, buffer = ((left, lefts), (right, rights))[side]
        return pltpu.make_async_copy(origin.at[task], buffer.at[task], sems.at[side, task])

    def start(sides, index, carry):
        for side in sides:
            copy(side, order[index]).start()
        return carry

    def arrive(side, task):
        if first:
            copy(side, task).wait()

    def rest(index, carry):
        for side in (0, 1):
            arrive(side, order[index])
        return carry

    def source(sector):
        return wave[sector]

    count = listed(targets, 1 - core[0], order, jnp.int32(0))
    listed(targets, core[0], order, count)
    if first:
        early = jnp.minimum(count, 2)
        lax.fori_loop(0, early, functools.partial(start, (0,)), 0)
        lax.fori_loop(0, early, functools.partial(start, (1,)), 0)
        lax.fori_loop(early, tasks, functools.partial(start, (0, 1)), 0)
        whole.wait()
    end = jnp.maximum(count, tasks // 2)
    clear(touched)
    run_tasks(targets, order, 0, count, source, lefts, rights, totals, touched, arrive)
    fill(totals, touched)
    out[...] = totals[...].astype(BF16)
    clear(touched)
    run_tasks(targets, order, count, end, source, lefts, rights, kept, touched, arrive)
    if first:
        lax.fori_loop(end, tasks, rest, 0)


def late_kernel(targets, core, vector, lefts, rights, begun, kept, touched, order):
    del begun
    tasks = lefts.shape[0]
    count = listed(targets, 1 - core[0], order, jnp.int32(0))
    listed(targets, core[0], order, count)
    end = jnp.maximum(count, tasks // 2)
    clear(touched)

    def mark(index, carry):
        touched[slot_of(targets, order[index])] = 1
        return carry

    def source(sector):
        return vector[sector]

    def arrive(side, task):
        del side, task

    lax.fori_loop(count, end, mark, 0)
    run_tasks(targets, order, end, tasks, source, lefts, rights, kept, touched, arrive)
    fill(kept, touched)


def apply_early(targets, core, vector, left, right, first):
    tasks, width, _ = left.shape
    slots = tasks // 2
    block = (slots, width, width)
    out = [jax.ShapeDtypeStruct(block, BF16), jax.ShapeDtypeStruct(block, F32)]
    scratch = [
        pltpu.SMEM((slots,), jnp.int32),
        pltpu.SMEM((tasks + 1,), jnp.int32),
        pltpu.VMEM(block, F32),
    ]
    if first:
        scratch += [
            pltpu.VMEM(vector.shape, BF16),
            pltpu.SMEM(targets.shape, jnp.int32),
            pltpu.SemaphoreType.DMA((2, tasks)),
            pltpu.SemaphoreType.DMA,
            pltpu.SemaphoreType.DMA,
        ]
        targets, vector, left, right = (
            pltpu.with_memory_space_constraint(value, pltpu.HBM)
            for value in (targets, vector, left, right)
        )
        out += [jax.ShapeDtypeStruct(left.shape, BF16)] * 2
    else:
        out += [jax.ShapeDtypeStruct((vector.shape[1], width, width), BF16)]
    return pl.pallas_call(
        functools.partial(early_kernel, first),
        out_shape=out,
        in_specs=[HBM, SMEM, HBM, HBM, HBM] if first else [SMEM, SMEM, VMEM, VMEM, VMEM],
        out_specs=[VMEM] * len(out),
        scratch_shapes=scratch,
        compiler_params=room(8),
        cost_estimate=work(tasks, width),
        name="early_first" if first else "early",
    )(targets, core, vector, left, right)


def apply_late(targets, core, vector, left, right, begun):
    tasks, width, _ = left.shape
    return pl.pallas_call(
        late_kernel,
        out_shape=jax.ShapeDtypeStruct(begun.shape, F32),
        in_specs=[SMEM, SMEM] + [VMEM] * 4,
        out_specs=VMEM,
        scratch_shapes=[
            pltpu.SMEM((tasks // 2,), jnp.int32),
            pltpu.SMEM((tasks + 1,), jnp.int32),
        ],
        input_output_aliases={5: 0},
        compiler_params=room(8),
        cost_estimate=work(tasks, width),
        name="late",
    )(targets, core, vector, left, right, begun)


def work(tasks, width):
    return pl.CostEstimate(
        flops=2 * tasks * width**3, bytes_accessed=2 * tasks * width**2, transcendentals=0
    )


def along_ring(value, step):
    pairs = []
    for op_0, op_1, op_2, half in itertools.product(range(2), range(4), range(4), range(2)):
        first, second = (op_1 + step) % 4, (op_2 + step) % 4
        pairs.append((place(op_0, op_1, op_2, half, 0), place(op_0, first, op_2, half, 0)))
        pairs.append((place(op_0, op_1, op_2, half, 1), place(op_0, op_1, second, half, 1)))
    return lax.ppermute(value, EVERY, pairs)


def across_rings(pieces):
    rest = REST_ORDER
    groups = [[place(low, ring, at, half, 0) for low, at, half in rest] for ring in range(4)]
    groups += [[place(low, at, ring, half, 1) for low, at, half in rest] for ring in range(4)]
    return exchange(pieces, groups)


def pack_kernel(ring, core, kept, arrived, own, *sent):
    others, local_sectors, rows, _ = own.shape
    near, far = rows, 4 * rows
    ring_stride = jnp.where(core[0] == 0, far, near)
    at_stride = jnp.where(core[0] == 0, near, far)
    to = [lax.rem(ring[0] + step, 4) * ring_stride for step in range(4)]

    def one_place(place, carry):
        base = place // 4 * (16 * rows) + lax.rem(place, 4) * at_stride
        for step, half, sector in itertools.product(range(4), range(2), range(local_sectors)):
            here = pl.ds(pl.multiple_of(base + to[step], rows), rows)
            slot = half * local_sectors + sector
            total = kept[slot, here, :] + arrived[slot, here, :].astype(F32)
            if step == 0:
                own[2 * place + half, sector] = total
            else:
                sent[step - 1][2 * place + half, sector] = total.astype(BF16)
        return carry

    lax.fori_loop(0, others // 2, one_place, 0)


def pack(ring, core, kept, arrived, shape):
    return pl.pallas_call(
        pack_kernel,
        out_shape=[jax.ShapeDtypeStruct(shape, F32)] + [jax.ShapeDtypeStruct(shape, BF16)] * 3,
        in_specs=[SMEM, SMEM, VMEM, VMEM],
        out_specs=[VMEM] * 4,
        compiler_params=room(4),
        name="pack",
    )(ring, core, kept, arrived)


def meet_kernel(own, first, second, third, out):
    for to, index in enumerate(REST_AT):
        total = own[index] + first[index].astype(F32)
        total += second[index].astype(F32) + third[index].astype(F32)
        out[to] = total.astype(BF16)


def meet(own, arrived):
    return pl.pallas_call(
        meet_kernel,
        out_shape=jax.ShapeDtypeStruct(own.shape, BF16),
        in_specs=[VMEM] * 4,
        out_specs=VMEM,
        compiler_params=room(4),
        name="meet",
    )(own, *arrived)


def summed(pieces):
    shape = pieces.shape[1:]
    count = pieces.shape[0]

    def add(index, total):
        return total + pieces[index].astype(F32)

    return lax.fori_loop(0, count, add, jnp.zeros(shape, F32), unroll=8)


def lanes(value):
    local_sectors, rows, width = value.shape
    flat = jnp.sum(value.reshape(local_sectors * rows, width), axis=0, keepdims=True)
    return sum(flat[:, at : at + 128] for at in range(0, width, 128))


def first_kernel(offset, pieces, wave, precond, sigma, again, sums):
    rows = precond.shape[1]
    own = wave[:, pl.ds(pl.multiple_of(offset[0], rows), rows), :].astype(F32)
    total = summed(pieces)
    sigma[...] = total
    again[...] = total
    ratio, scaled = total / precond[...], own / precond[...]
    terms = (
        own * own,
        own * total,
        own * ratio,
        own * scaled,
        ratio * ratio,
        ratio * scaled,
        scaled * scaled,
    )
    one = jnp.concatenate([lanes(term) for term in terms] + [jnp.zeros((1, 128), F32)], axis=0)
    one = jnp.sum(one, axis=1, keepdims=True)
    row = lax.broadcasted_iota(jnp.int32, (8, 128), 0)
    lane = lax.broadcasted_iota(jnp.int32, (8, 128), 1)
    one = jnp.sum(jnp.where(row == lane, one, 0.0), axis=0, keepdims=True)
    sums[...] = jnp.broadcast_to(one[None], sums.shape)


def second_kernel(offset, sums, sigma, wave, precond, copies):
    rows = precond.shape[1]
    own = wave[:, pl.ds(pl.multiple_of(offset[0], rows), rows), :].astype(F32)
    whole = summed(sums)
    norm_sq, w_s, w_r, w_b, r_r, r_b, b_b = (whole[:, k : k + 1] for k in range(7))
    shift = w_s / norm_sq - 1.0
    projected = w_r - shift * w_b
    correction_sq = r_r - 2.0 * shift * r_b + shift * shift * b_b
    along = projected / norm_sq
    update_sq = jnp.maximum(correction_sq - projected * along, 0.0)
    scale = jnp.sqrt(norm_sq) * lax.rsqrt(update_sq + 1e-06)
    correction = (sigma[...] - shift[None] * own) / precond[...]
    new = ((correction - along[None] * own) * scale[None]).astype(BF16)
    copies[...] = jnp.broadcast_to(new[None], copies.shape)


def sum_kernel(pieces, sigma):
    sigma[...] = summed(pieces)


def on_device(wavefunction, left_blocks, right_blocks, target_sector, preconditioner):
    local_sectors, width, _ = wavefunction.shape
    rows = preconditioner.shape[1]
    owners = lax.axis_size(OP)
    offset = (lax.axis_index(OP) * rows).reshape(1)
    mine = lax.axis_index(CORE).reshape(1)
    ring = jnp.where(mine == 0, lax.axis_index("op_1"), lax.axis_index("op_2"))
    targets = target_sector.T
    left, right = (
        blocks.reshape(-1, width, width) for blocks in (left_blocks, right_blocks)
    )
    row_shape = jax.ShapeDtypeStruct((local_sectors, rows, width), F32)
    offset, mine, ring = lax.optimization_barrier((offset, mine, ring))

    def partial_pieces(vector, left, right, first):
        sent, begun, *rest = apply_early(targets, mine, vector, left, right, first)
        if first:
            left, right = rest
        else:
            (vector,) = rest
        arrived = lax.ppermute(sent, CORE, [(0, 1), (1, 0)])
        kept = apply_late(targets, mine, vector, left, right, begun)
        shape = (owners // 2, local_sectors, rows, width)
        own, *sent = pack(ring, mine, kept, arrived, shape)
        arrived = [along_ring(sent[step - 1], step) for step in (2, 1, 3)]
        return across_rings(meet(own, arrived)), left, right

    pieces, left, right = partial_pieces(wavefunction, left, right, True)
    devices = lax.axis_size(EVERY)
    sigma_first, again, sums = pl.pallas_call(
        first_kernel,
        out_shape=(row_shape, row_shape, jax.ShapeDtypeStruct((devices, 1, 128), F32)),
        in_specs=[SMEM, VMEM, VMEM, VMEM],
        out_specs=(VMEM, VMEM, VMEM),
        compiler_params=room(4),
        name="first",
    )(offset, pieces, wavefunction, preconditioner)
    sums = with_everyone(sums)
    copies = pl.pallas_call(
        second_kernel,
        out_shape=jax.ShapeDtypeStruct((owners, local_sectors, rows, width), BF16),
        in_specs=[SMEM, VMEM, VMEM, VMEM, VMEM],
        out_specs=VMEM,
        compiler_params=room(4),
        name="second",
    )(offset, sums, again, wavefunction, preconditioner)
    pieces, _, _ = partial_pieces(over_terms(copies), left, right, False)
    sigma_second = pl.pallas_call(
        sum_kernel,
        out_shape=row_shape,
        in_specs=[VMEM],
        out_specs=VMEM,
        compiler_params=room(4),
        name="last",
    )(pieces)
    return (sigma_first, sigma_second)


def solution(mesh):
    torus = Mesh(mesh.devices.reshape(2, 4, 4, 2, 2), EVERY)
    placed = (
        P(SECTOR, None, None),
        P(OP, SECTOR, None, None),
        P(OP, SECTOR, None, None),
        P(OP, SECTOR),
        P(SECTOR, OP, None),
    )
    return jax.shard_map(
        on_device,
        mesh=torus,
        in_specs=placed,
        out_specs=(P(SECTOR, OP, None), P(SECTOR, OP, None)),
        check_vma=False,
    )
```

```python
import functools
import itertools
import random

import jax
import jax.numpy as jnp
from jax import lax
from jax.experimental import pallas as pl
from jax.experimental.pallas import tpu as pltpu
from jax.sharding import Mesh
from jax.sharding import PartitionSpec as P

SECTOR = ("sector_0", "sector_1")
OP = ("op_0", "op_1", "op_2")
EVERY = ("op_0", "op_1", "op_2", "sector_0", "sector_1")
CORE = "sector_1"
F32 = jnp.float32
BF16 = jnp.bfloat16
VMEM = pl.BlockSpec(memory_space=pltpu.VMEM)
SMEM = pl.BlockSpec(memory_space=pltpu.SMEM)
HBM = pl.BlockSpec(memory_space=pltpu.HBM)


def room(mebibytes):
    return pltpu.CompilerParams(vmem_limit_bytes=mebibytes * 2**20)


def place(op_0, op_1, op_2, half, core):
    return (((op_0 * 4 + op_1) * 4 + op_2) * 2 + half) * 2 + core


def mixed(members, seed):
    members = list(members)
    random.Random(seed).shuffle(members)
    return members


OP_ORDER = list(itertools.product(range(2), range(4), range(4)))
REST_ORDER = mixed(itertools.product(range(2), range(4), range(2)), 3)
REST_AT = [(low * 4 + at) * 2 + half for low, at, half in REST_ORDER]


def exchange(pieces, groups):
    return lax.all_to_all(
        pieces, EVERY, split_axis=0, concat_axis=0, axis_index_groups=groups, tiled=True
    )


def with_everyone(pieces):
    return exchange(pieces, [list(range(lax.axis_size(EVERY)))])


def over_terms(pieces):
    sectors = itertools.product(range(2), range(2))
    return exchange(
        pieces, [[place(*op, half, core) for op in OP_ORDER] for half, core in sectors]
    )


def listed(targets, core, order, at):
    local_sectors, terms = targets.shape

    def scan(task, count):
        target = targets[lax.rem(task, local_sectors), task // local_sectors]
        order[count] = task
        return count + (lax.rem(target // local_sectors, 2) == core).astype(jnp.int32)

    return lax.fori_loop(0, local_sectors * terms, scan, at)


def slot_of(targets, task):
    local_sectors = targets.shape[0]
    target = targets[lax.rem(task, local_sectors), task // local_sectors]
    return target // (2 * local_sectors) * local_sectors + lax.rem(target, local_sectors)


def run_tasks(targets, order, begin, end, source, lefts, rights, totals, touched, arrive):
    local_sectors = targets.shape[0]

    def middle_of(task):
        vector = source(lax.rem(task, local_sectors))
        return jnp.dot(lefts[task], vector, preferred_element_type=F32).astype(BF16)

    def add(task, middle):
        slot = slot_of(targets, task)
        fresh = touched[slot] == 0
        touched[slot] = 1
        share = lax.dot_general(
            middle, rights[task], (((1,), (1,)), ((), ())), preferred_element_type=F32
        )
        totals[slot] = share + jnp.where(fresh, 0.0, totals[slot])

    def pair(index, carry):
        tasks = order[begin + 2 * index], order[begin + 2 * index + 1]
        for task in tasks:
            arrive(0, task)
        middles = [middle_of(task) for task in tasks]
        for task in tasks:
            arrive(1, task)
        for task, middle in zip(tasks, middles):
            add(task, middle)
        return carry

    lax.fori_loop(0, (end - begin) // 2, pair, 0)

    @pl.when(lax.rem(end - begin, 2) == 1)
    def _():
        task = order[end - 1]
        arrive(0, task)
        arrive(1, task)
        add(task, middle_of(task))


def clear(touched):
    for slot in range(touched.shape[0]):
        touched[slot] = 0


def fill(totals, touched):
    for slot in range(totals.shape[0]):

        @pl.when(touched[slot] == 0)
        def _(slot=slot):
            totals[slot] = jnp.zeros(totals.shape[1:], F32)


def early_kernel(first, targets, core, vector, left, right, out, kept, *refs):
    if first:
        lefts, rights, touched, order, totals, wave, known, sems, wave_sem, known_sem = refs
        whole = pltpu.make_async_copy(vector, wave, wave_sem)
        listing = pltpu.make_async_copy(targets, known, known_sem)
        listing.start()
        whole.start()
        listing.wait()
        targets = known
    else:
        lefts, rights = left, right
        touched, order, totals = refs
    tasks = lefts.shape[0]

    def copy(side, task):
        origin, buffer = ((left, lefts), (right, rights))[side]
        return pltpu.make_async_copy(origin.at[task], buffer.at[task], sems.at[side, task])

    def start(sides, index, carry):
        for side in sides:
            copy(side, order[index]).start()
        return carry

    def arrive(side, task):
        if first:
            copy(side, task).wait()

    def rest(index, carry):
        for side in (0, 1):
            arrive(side, order[index])
        return carry

    def source(sector):
        return wave[sector] if first else vector[:, sector].reshape(lefts.shape[1:])

    count = listed(targets, 1 - core[0], order, jnp.int32(0))
    listed(targets, core[0], order, count)
    if first:
        early = jnp.minimum(count, 2)
        lax.fori_loop(0, early, functools.partial(start, (0,)), 0)
        lax.fori_loop(0, early, functools.partial(start, (1,)), 0)
        lax.fori_loop(early, tasks, functools.partial(start, (0, 1)), 0)
        whole.wait()
    end = jnp.maximum(count, tasks // 2)
    clear(touched)
    run_tasks(targets, order, 0, count, source, lefts, rights, totals, touched, arrive)
    fill(totals, touched)
    out[...] = totals[...].astype(BF16)
    clear(touched)
    run_tasks(targets, order, count, end, source, lefts, rights, kept, touched, arrive)
    if first:
        lax.fori_loop(end, tasks, rest, 0)


def late_kernel(targets, core, vector, lefts, rights, begun, kept, touched, order):
    del begun
    tasks = lefts.shape[0]
    count = listed(targets, 1 - core[0], order, jnp.int32(0))
    listed(targets, core[0], order, count)
    end = jnp.maximum(count, tasks // 2)
    clear(touched)

    def mark(index, carry):
        touched[slot_of(targets, order[index])] = 1
        return carry

    def source(sector):
        whole = vector[sector] if vector.shape[1:] == lefts.shape[1:] else vector[:, sector]
        return whole.reshape(lefts.shape[1:])

    def arrive(side, task):
        del side, task

    lax.fori_loop(count, end, mark, 0)
    run_tasks(targets, order, end, tasks, source, lefts, rights, kept, touched, arrive)
    fill(kept, touched)


def apply_early(targets, core, vector, left, right, first):
    tasks, width, _ = left.shape
    slots = tasks // 2
    block = (slots, width, width)
    out = [jax.ShapeDtypeStruct(block, BF16), jax.ShapeDtypeStruct(block, F32)]
    scratch = [
        pltpu.SMEM((slots,), jnp.int32),
        pltpu.SMEM((tasks + 1,), jnp.int32),
        pltpu.VMEM(block, F32),
    ]
    if first:
        scratch += [
            pltpu.VMEM(vector.shape, BF16),
            pltpu.SMEM(targets.shape, jnp.int32),
            pltpu.SemaphoreType.DMA((2, tasks)),
            pltpu.SemaphoreType.DMA,
            pltpu.SemaphoreType.DMA,
        ]
        targets, vector, left, right = (
            pltpu.with_memory_space_constraint(value, pltpu.HBM)
            for value in (targets, vector, left, right)
        )
        out += [jax.ShapeDtypeStruct(left.shape, BF16)] * 2
    return pl.pallas_call(
        functools.partial(early_kernel, first),
        out_shape=out,
        in_specs=[HBM, SMEM, HBM, HBM, HBM] if first else [SMEM, SMEM, VMEM, VMEM, VMEM],
        out_specs=[VMEM] * len(out),
        scratch_shapes=scratch,
        compiler_params=room(8),
        cost_estimate=work(tasks, width),
        name="early_first" if first else "early",
    )(targets, core, vector, left, right)


def apply_late(targets, core, vector, left, right, begun):
    tasks, width, _ = left.shape
    return pl.pallas_call(
        late_kernel,
        out_shape=jax.ShapeDtypeStruct(begun.shape, F32),
        in_specs=[SMEM, SMEM] + [VMEM] * 4,
        out_specs=VMEM,
        scratch_shapes=[
            pltpu.SMEM((tasks // 2,), jnp.int32),
            pltpu.SMEM((tasks + 1,), jnp.int32),
        ],
        input_output_aliases={5: 0},
        compiler_params=room(8),
        cost_estimate=work(tasks, width),
        name="late",
    )(targets, core, vector, left, right, begun)


def work(tasks, width):
    return pl.CostEstimate(
        flops=2 * tasks * width**3, bytes_accessed=2 * tasks * width**2, transcendentals=0
    )


def along_ring(value, step):
    pairs = []
    for op_0, op_1, op_2, half in itertools.product(range(2), range(4), range(4), range(2)):
        first, second = (op_1 + step) % 4, (op_2 + step) % 4
        pairs.append((place(op_0, op_1, op_2, half, 0), place(op_0, first, op_2, half, 0)))
        pairs.append((place(op_0, op_1, op_2, half, 1), place(op_0, op_1, second, half, 1)))
    return lax.ppermute(value, EVERY, pairs)


def across_rings(pieces):
    rest = REST_ORDER
    groups = [[place(low, ring, at, half, 0) for low, at, half in rest] for ring in range(4)]
    groups += [[place(low, at, ring, half, 1) for low, at, half in rest] for ring in range(4)]
    return exchange(pieces, groups)


def pack_kernel(ring, core, kept, arrived, own, *sent):
    others, local_sectors, rows, _ = own.shape
    near, far = rows, 4 * rows
    ring_stride = jnp.where(core[0] == 0, far, near)
    at_stride = jnp.where(core[0] == 0, near, far)
    to = [lax.rem(ring[0] + step, 4) * ring_stride for step in range(4)]

    def one_place(place, carry):
        base = place // 4 * (16 * rows) + lax.rem(place, 4) * at_stride
        for step, half, sector in itertools.product(range(4), range(2), range(local_sectors)):
            here = pl.ds(pl.multiple_of(base + to[step], rows), rows)
            slot = half * local_sectors + sector
            total = kept[slot, here, :] + arrived[slot, here, :].astype(F32)
            if step == 0:
                own[2 * place + half, sector] = total
            else:
                sent[step - 1][2 * place + half, sector] = total.astype(BF16)
        return carry

    lax.fori_loop(0, others // 2, one_place, 0)


def pack(ring, core, kept, arrived, shape):
    return pl.pallas_call(
        pack_kernel,
        out_shape=[jax.ShapeDtypeStruct(shape, F32)] + [jax.ShapeDtypeStruct(shape, BF16)] * 3,
        in_specs=[SMEM, SMEM, VMEM, VMEM],
        out_specs=[VMEM] * 4,
        compiler_params=room(4),
        name="pack",
    )(ring, core, kept, arrived)


def meet_kernel(own, first, second, third, out):
    for to, index in enumerate(REST_AT):
        total = own[index] + first[index].astype(F32)
        total += second[index].astype(F32) + third[index].astype(F32)
        out[to] = total.astype(BF16)


def meet(own, arrived):
    return pl.pallas_call(
        meet_kernel,
        out_shape=jax.ShapeDtypeStruct(own.shape, BF16),
        in_specs=[VMEM] * 4,
        out_specs=VMEM,
        compiler_params=room(4),
        name="meet",
    )(own, *arrived)


def summed(pieces):
    shape = pieces.shape[1:]
    count = pieces.shape[0]

    def add(index, total):
        return total + pieces[index].astype(F32)

    return lax.fori_loop(0, count, add, jnp.zeros(shape, F32), unroll=8)


def lanes(value):
    local_sectors, rows, width = value.shape
    flat = jnp.sum(value.reshape(local_sectors * rows, width), axis=0, keepdims=True)
    return sum(flat[:, at : at + 128] for at in range(0, width, 128))


def first_kernel(offset, pieces, wave, precond, sigma, again, sums):
    rows = precond.shape[1]
    own = wave[:, pl.ds(pl.multiple_of(offset[0], rows), rows), :].astype(F32)
    total = summed(pieces)
    sigma[...] = total
    again[...] = total
    ratio, scaled = total / precond[...], own / precond[...]
    terms = (
        own * own,
        own * total,
        own * ratio,
        own * scaled,
        ratio * ratio,
        ratio * scaled,
        scaled * scaled,
    )
    one = jnp.concatenate([lanes(term) for term in terms] + [jnp.zeros((1, 128), F32)], axis=0)
    one = jnp.sum(one, axis=1, keepdims=True)
    row = lax.broadcasted_iota(jnp.int32, (8, 128), 0)
    lane = lax.broadcasted_iota(jnp.int32, (8, 128), 1)
    one = jnp.sum(jnp.where(row == lane, one, 0.0), axis=0, keepdims=True)
    sums[...] = jnp.broadcast_to(one[None], sums.shape)


def second_kernel(offset, sums, sigma, wave, precond, copies):
    rows = precond.shape[1]
    own = wave[:, pl.ds(pl.multiple_of(offset[0], rows), rows), :].astype(F32)
    whole = summed(sums)
    norm_sq, w_s, w_r, w_b, r_r, r_b, b_b = (whole[:, k : k + 1] for k in range(7))
    shift = w_s / norm_sq - 1.0
    projected = w_r - shift * w_b
    correction_sq = r_r - 2.0 * shift * r_b + shift * shift * b_b
    along = projected / norm_sq
    update_sq = jnp.maximum(correction_sq - projected * along, 0.0)
    scale = jnp.sqrt(norm_sq) * lax.rsqrt(update_sq + 1e-06)
    correction = (sigma[...] - shift[None] * own) / precond[...]
    new = ((correction - along[None] * own) * scale[None]).astype(BF16)
    copies[...] = jnp.broadcast_to(new[None], copies.shape)


def sum_kernel(pieces, sigma):
    sigma[...] = summed(pieces)


def on_device(wavefunction, left_blocks, right_blocks, target_sector, preconditioner):
    local_sectors, width, _ = wavefunction.shape
    rows = preconditioner.shape[1]
    owners = lax.axis_size(OP)
    offset = (lax.axis_index(OP) * rows).reshape(1)
    mine = lax.axis_index(CORE).reshape(1)
    ring = jnp.where(mine == 0, lax.axis_index("op_1"), lax.axis_index("op_2"))
    targets = target_sector.T
    left, right = (
        blocks.reshape(-1, width, width) for blocks in (left_blocks, right_blocks)
    )
    row_shape = jax.ShapeDtypeStruct((local_sectors, rows, width), F32)
    offset, mine, ring = lax.optimization_barrier((offset, mine, ring))

    def partial_pieces(vector, left, right, first):
        sent, begun, *blocks = apply_early(targets, mine, vector, left, right, first)
        left, right = blocks if first else (left, right)
        arrived = lax.ppermute(sent, CORE, [(0, 1), (1, 0)])
        kept = apply_late(targets, mine, vector, left, right, begun)
        shape = (owners // 2, local_sectors, rows, width)
        own, *sent = pack(ring, mine, kept, arrived, shape)
        arrived = [along_ring(sent[step - 1], step) for step in (2, 1, 3)]
        return across_rings(meet(own, arrived)), left, right

    pieces, left, right = partial_pieces(wavefunction, left, right, True)
    devices = lax.axis_size(EVERY)
    sigma_first, again, sums = pl.pallas_call(
        first_kernel,
        out_shape=(row_shape, row_shape, jax.ShapeDtypeStruct((devices, 1, 128), F32)),
        in_specs=[SMEM, VMEM, VMEM, VMEM],
        out_specs=(VMEM, VMEM, VMEM),
        compiler_params=room(4),
        name="first",
    )(offset, pieces, wavefunction, preconditioner)
    sums = with_everyone(sums)
    copies = pl.pallas_call(
        second_kernel,
        out_shape=jax.ShapeDtypeStruct((owners, local_sectors, rows, width), BF16),
        in_specs=[SMEM, VMEM, VMEM, VMEM, VMEM],
        out_specs=VMEM,
        compiler_params=room(4),
        name="second",
    )(offset, sums, again, wavefunction, preconditioner)
    pieces, _, _ = partial_pieces(over_terms(copies), left, right, False)
    sigma_second = pl.pallas_call(
        sum_kernel,
        out_shape=row_shape,
        in_specs=[VMEM],
        out_specs=VMEM,
        compiler_params=room(4),
        name="last",
    )(pieces)
    return (sigma_first, sigma_second)


def solution(mesh):
    torus = Mesh(mesh.devices.reshape(2, 4, 4, 2, 2), EVERY)
    placed = (
        P(SECTOR, None, None),
        P(OP, SECTOR, None, None),
        P(OP, SECTOR, None, None),
        P(OP, SECTOR),
        P(SECTOR, OP, None),
    )
    return jax.shard_map(
        on_device,
        mesh=torus,
        in_specs=placed,
        out_specs=(P(SECTOR, OP, None), P(SECTOR, OP, None)),
        check_vma=False,
    )
```

```python
import functools
import itertools
import random

import jax
import jax.numpy as jnp
from jax import lax
from jax.experimental import pallas as pl
from jax.experimental.pallas import tpu as pltpu
from jax.sharding import Mesh
from jax.sharding import PartitionSpec as P

SECTOR = ("sector_0", "sector_1")
OP = ("op_0", "op_1", "op_2")
EVERY = ("op_0", "op_1", "op_2", "sector_0", "sector_1")
CORE = "sector_1"
F32 = jnp.float32
BF16 = jnp.bfloat16
VMEM = pl.BlockSpec(memory_space=pltpu.VMEM)
SMEM = pl.BlockSpec(memory_space=pltpu.SMEM)
HBM = pl.BlockSpec(memory_space=pltpu.HBM)


def room(mebibytes):
    return pltpu.CompilerParams(vmem_limit_bytes=mebibytes * 2**20)


def place(op_0, op_1, op_2, half, core):
    return (((op_0 * 4 + op_1) * 4 + op_2) * 2 + half) * 2 + core


def mixed(members, seed):
    members = list(members)
    random.Random(seed).shuffle(members)
    return members


OP_ORDER = list(itertools.product(range(2), range(4), range(4)))
REST_ORDER = mixed(itertools.product(range(2), range(4), range(2)), 3)
REST_AT = [(low * 4 + at) * 2 + half for low, at, half in REST_ORDER]


def exchange(pieces, groups):
    return lax.all_to_all(
        pieces, EVERY, split_axis=0, concat_axis=0, axis_index_groups=groups, tiled=True
    )


def with_everyone(pieces):
    return exchange(pieces, [mixed(range(lax.axis_size(EVERY)), 0)])


def over_terms(pieces):
    sectors = itertools.product(range(2), range(2))
    return exchange(
        pieces, [[place(*op, half, core) for op in OP_ORDER] for half, core in sectors]
    )


def listed(targets, core, order, at):
    local_sectors, terms = targets.shape

    def scan(task, count):
        target = targets[lax.rem(task, local_sectors), task // local_sectors]
        order[count] = task
        return count + (lax.rem(target // local_sectors, 2) == core).astype(jnp.int32)

    return lax.fori_loop(0, local_sectors * terms, scan, at)


def slot_of(targets, task):
    local_sectors = targets.shape[0]
    target = targets[lax.rem(task, local_sectors), task // local_sectors]
    return target // (2 * local_sectors) * local_sectors + lax.rem(target, local_sectors)


def run_tasks(targets, order, begin, end, source, lefts, rights, totals, touched, arrive):
    local_sectors = targets.shape[0]

    def middle_of(task):
        vector = source(lax.rem(task, local_sectors))
        return jnp.dot(lefts[task], vector, preferred_element_type=F32).astype(BF16)

    def add(task, middle):
        slot = slot_of(targets, task)
        fresh = touched[slot] == 0
        touched[slot] = 1
        share = lax.dot_general(
            middle, rights[task], (((1,), (1,)), ((), ())), preferred_element_type=F32
        )
        totals[slot] = share + jnp.where(fresh, 0.0, totals[slot])

    def pair(index, carry):
        tasks = order[begin + 2 * index], order[begin + 2 * index + 1]
        for task in tasks:
            arrive(0, task)
        middles = [middle_of(task) for task in tasks]
        for task in tasks:
            arrive(1, task)
        for task, middle in zip(tasks, middles):
            add(task, middle)
        return carry

    lax.fori_loop(0, (end - begin) // 2, pair, 0)

    @pl.when(lax.rem(end - begin, 2) == 1)
    def _():
        task = order[end - 1]
        arrive(0, task)
        arrive(1, task)
        add(task, middle_of(task))


def clear(touched):
    for slot in range(touched.shape[0]):
        touched[slot] = 0


def fill(totals, touched):
    for slot in range(totals.shape[0]):

        @pl.when(touched[slot] == 0)
        def _(slot=slot):
            totals[slot] = jnp.zeros(totals.shape[1:], F32)


def early_kernel(first, targets, core, vector, left, right, out, kept, *refs):
    if first:
        lefts, rights, touched, order, totals, wave, known, sems, wave_sem, known_sem = refs
        whole = pltpu.make_async_copy(vector, wave, wave_sem)
        listing = pltpu.make_async_copy(targets, known, known_sem)
        listing.start()
        whole.start()
        listing.wait()
        targets = known
    else:
        lefts, rights = left, right
        touched, order, totals = refs
    tasks = lefts.shape[0]

    def copy(side, task):
        origin, buffer = ((left, lefts), (right, rights))[side]
        return pltpu.make_async_copy(origin.at[task], buffer.at[task], sems.at[side, task])

    def start(sides, index, carry):
        for side in sides:
            copy(side, order[index]).start()
        return carry

    def arrive(side, task):
        if first:
            copy(side, task).wait()

    def rest(index, carry):
        for side in (0, 1):
            arrive(side, order[index])
        return carry

    def source(sector):
        return wave[sector] if first else vector[:, sector].reshape(lefts.shape[1:])

    count = listed(targets, 1 - core[0], order, jnp.int32(0))
    listed(targets, core[0], order, count)
    if first:
        early = jnp.minimum(count, 2)
        lax.fori_loop(0, early, functools.partial(start, (0,)), 0)
        lax.fori_loop(0, early, functools.partial(start, (1,)), 0)
        lax.fori_loop(early, tasks, functools.partial(start, (0, 1)), 0)
        whole.wait()
    end = jnp.maximum(count, tasks // 2)
    clear(touched)
    run_tasks(targets, order, 0, count, source, lefts, rights, totals, touched, arrive)
    fill(totals, touched)
    out[...] = totals[...].astype(BF16)
    clear(touched)
    run_tasks(targets, order, count, end, source, lefts, rights, kept, touched, arrive)
    if first:
        lax.fori_loop(end, tasks, rest, 0)


def late_kernel(targets, core, vector, lefts, rights, begun, kept, touched, order):
    del begun
    tasks = lefts.shape[0]
    count = listed(targets, 1 - core[0], order, jnp.int32(0))
    listed(targets, core[0], order, count)
    end = jnp.maximum(count, tasks // 2)
    clear(touched)

    def mark(index, carry):
        touched[slot_of(targets, order[index])] = 1
        return carry

    def source(sector):
        whole = vector[sector] if vector.shape[1:] == lefts.shape[1:] else vector[:, sector]
        return whole.reshape(lefts.shape[1:])

    def arrive(side, task):
        del side, task

    lax.fori_loop(count, end, mark, 0)
    run_tasks(targets, order, end, tasks, source, lefts, rights, kept, touched, arrive)
    fill(kept, touched)


def apply_early(targets, core, vector, left, right, first):
    tasks, width, _ = left.shape
    slots = tasks // 2
    block = (slots, width, width)
    out = [jax.ShapeDtypeStruct(block, BF16), jax.ShapeDtypeStruct(block, F32)]
    scratch = [
        pltpu.SMEM((slots,), jnp.int32),
        pltpu.SMEM((tasks + 1,), jnp.int32),
        pltpu.VMEM(block, F32),
    ]
    if first:
        scratch += [
            pltpu.VMEM(vector.shape, BF16),
            pltpu.SMEM(targets.shape, jnp.int32),
            pltpu.SemaphoreType.DMA((2, tasks)),
            pltpu.SemaphoreType.DMA,
            pltpu.SemaphoreType.DMA,
        ]
        targets, vector, left, right = (
            pltpu.with_memory_space_constraint(value, pltpu.HBM)
            for value in (targets, vector, left, right)
        )
        out += [jax.ShapeDtypeStruct(left.shape, BF16)] * 2
    return pl.pallas_call(
        functools.partial(early_kernel, first),
        out_shape=out,
        in_specs=[HBM, SMEM, HBM, HBM, HBM] if first else [SMEM, SMEM, VMEM, VMEM, VMEM],
        out_specs=[VMEM] * len(out),
        scratch_shapes=scratch,
        compiler_params=room(8),
        cost_estimate=work(tasks, width),
        name="early_first" if first else "early",
    )(targets, core, vector, left, right)


def apply_late(targets, core, vector, left, right, begun):
    tasks, width, _ = left.shape
    return pl.pallas_call(
        late_kernel,
        out_shape=jax.ShapeDtypeStruct(begun.shape, F32),
        in_specs=[SMEM, SMEM] + [VMEM] * 4,
        out_specs=VMEM,
        scratch_shapes=[
            pltpu.SMEM((tasks // 2,), jnp.int32),
            pltpu.SMEM((tasks + 1,), jnp.int32),
        ],
        input_output_aliases={5: 0},
        compiler_params=room(8),
        cost_estimate=work(tasks, width),
        name="late",
    )(targets, core, vector, left, right, begun)


def work(tasks, width):
    return pl.CostEstimate(
        flops=2 * tasks * width**3, bytes_accessed=2 * tasks * width**2, transcendentals=0
    )


def along_ring(value, step):
    pairs = []
    for op_0, op_1, op_2, half in itertools.product(range(2), range(4), range(4), range(2)):
        first, second = (op_1 + step) % 4, (op_2 + step) % 4
        pairs.append((place(op_0, op_1, op_2, half, 0), place(op_0, first, op_2, half, 0)))
        pairs.append((place(op_0, op_1, op_2, half, 1), place(op_0, op_1, second, half, 1)))
    return lax.ppermute(value, EVERY, pairs)


def across_rings(pieces):
    rest = REST_ORDER
    groups = [[place(low, ring, at, half, 0) for low, at, half in rest] for ring in range(4)]
    groups += [[place(low, at, ring, half, 1) for low, at, half in rest] for ring in range(4)]
    return exchange(pieces, groups)


def pack_kernel(ring, core, kept, arrived, own, *sent):
    others, local_sectors, rows, _ = own.shape
    near, far = rows, 4 * rows
    ring_stride = jnp.where(core[0] == 0, far, near)
    at_stride = jnp.where(core[0] == 0, near, far)
    to = [lax.rem(ring[0] + step, 4) * ring_stride for step in range(4)]

    def one_place(place, carry):
        base = place // 4 * (16 * rows) + lax.rem(place, 4) * at_stride
        for step, half, sector in itertools.product(range(4), range(2), range(local_sectors)):
            here = pl.ds(pl.multiple_of(base + to[step], rows), rows)
            slot = half * local_sectors + sector
            total = kept[slot, here, :] + arrived[slot, here, :].astype(F32)
            if step == 0:
                own[2 * place + half, sector] = total
            else:
                sent[step - 1][2 * place + half, sector] = total.astype(BF16)
        return carry

    lax.fori_loop(0, others // 2, one_place, 0)


def pack(ring, core, kept, arrived, shape):
    return pl.pallas_call(
        pack_kernel,
        out_shape=[jax.ShapeDtypeStruct(shape, F32)] + [jax.ShapeDtypeStruct(shape, BF16)] * 3,
        in_specs=[SMEM, SMEM, VMEM, VMEM],
        out_specs=[VMEM] * 4,
        compiler_params=room(4),
        name="pack",
    )(ring, core, kept, arrived)


def meet_kernel(own, first, second, third, out):
    for to, index in enumerate(REST_AT):
        total = own[index] + first[index].astype(F32)
        total += second[index].astype(F32) + third[index].astype(F32)
        out[to] = total.astype(BF16)


def meet(own, arrived):
    return pl.pallas_call(
        meet_kernel,
        out_shape=jax.ShapeDtypeStruct(own.shape, BF16),
        in_specs=[VMEM] * 4,
        out_specs=VMEM,
        compiler_params=room(4),
        name="meet",
    )(own, *arrived)


def summed(pieces):
    shape = pieces.shape[1:]
    count = pieces.shape[0]

    def add(index, total):
        return total + pieces[index].astype(F32)

    return lax.fori_loop(0, count, add, jnp.zeros(shape, F32), unroll=8)


def lanes(value):
    local_sectors, rows, width = value.shape
    flat = jnp.sum(value.reshape(local_sectors * rows, width), axis=0, keepdims=True)
    return sum(flat[:, at : at + 128] for at in range(0, width, 128))


def first_kernel(offset, pieces, wave, precond, sigma, again, sums):
    rows = precond.shape[1]
    own = wave[:, pl.ds(pl.multiple_of(offset[0], rows), rows), :].astype(F32)
    total = summed(pieces)
    sigma[...] = total
    again[...] = total
    ratio, scaled = total / precond[...], own / precond[...]
    terms = (
        own * own,
        own * total,
        own * ratio,
        own * scaled,
        ratio * ratio,
        ratio * scaled,
        scaled * scaled,
    )
    one = jnp.concatenate([lanes(term) for term in terms] + [jnp.zeros((1, 128), F32)], axis=0)
    one = jnp.sum(one, axis=1, keepdims=True)
    row = lax.broadcasted_iota(jnp.int32, (8, 128), 0)
    lane = lax.broadcasted_iota(jnp.int32, (8, 128), 1)
    one = jnp.sum(jnp.where(row == lane, one, 0.0), axis=0, keepdims=True)
    sums[...] = jnp.broadcast_to(one[None], sums.shape)


def second_kernel(offset, sums, sigma, wave, precond, copies):
    rows = precond.shape[1]
    own = wave[:, pl.ds(pl.multiple_of(offset[0], rows), rows), :].astype(F32)
    whole = summed(sums)
    norm_sq, w_s, w_r, w_b, r_r, r_b, b_b = (whole[:, k : k + 1] for k in range(7))
    shift = w_s / norm_sq - 1.0
    projected = w_r - shift * w_b
    correction_sq = r_r - 2.0 * shift * r_b + shift * shift * b_b
    along = projected / norm_sq
    update_sq = jnp.maximum(correction_sq - projected * along, 0.0)
    scale = jnp.sqrt(norm_sq) * lax.rsqrt(update_sq + 1e-06)
    correction = (sigma[...] - shift[None] * own) / precond[...]
    new = ((correction - along[None] * own) * scale[None]).astype(BF16)
    copies[...] = jnp.broadcast_to(new[None], copies.shape)


def sum_kernel(pieces, sigma):
    sigma[...] = summed(pieces)


def on_device(wavefunction, left_blocks, right_blocks, target_sector, preconditioner):
    local_sectors, width, _ = wavefunction.shape
    rows = preconditioner.shape[1]
    owners = lax.axis_size(OP)
    offset = (lax.axis_index(OP) * rows).reshape(1)
    mine = lax.axis_index(CORE).reshape(1)
    ring = jnp.where(mine == 0, lax.axis_index("op_1"), lax.axis_index("op_2"))
    targets = target_sector.T
    left, right = (
        blocks.reshape(-1, width, width) for blocks in (left_blocks, right_blocks)
    )
    row_shape = jax.ShapeDtypeStruct((local_sectors, rows, width), F32)
    offset, mine, ring = lax.optimization_barrier((offset, mine, ring))

    def partial_pieces(vector, left, right, first):
        sent, begun, *blocks = apply_early(targets, mine, vector, left, right, first)
        left, right = blocks if first else (left, right)
        arrived = lax.ppermute(sent, CORE, [(0, 1), (1, 0)])
        kept = apply_late(targets, mine, vector, left, right, begun)
        shape = (owners // 2, local_sectors, rows, width)
        own, *sent = pack(ring, mine, kept, arrived, shape)
        arrived = [along_ring(sent[step - 1], step) for step in (2, 1, 3)]
        return across_rings(meet(own, arrived)), left, right

    pieces, left, right = partial_pieces(wavefunction, left, right, True)
    devices = lax.axis_size(EVERY)
    sigma_first, again, sums = pl.pallas_call(
        first_kernel,
        out_shape=(row_shape, row_shape, jax.ShapeDtypeStruct((devices, 1, 128), F32)),
        in_specs=[SMEM, VMEM, VMEM, VMEM],
        out_specs=(VMEM, VMEM, VMEM),
        compiler_params=room(4),
        name="first",
    )(offset, pieces, wavefunction, preconditioner)
    sums = with_everyone(sums)
    copies = pl.pallas_call(
        second_kernel,
        out_shape=jax.ShapeDtypeStruct((owners, local_sectors, rows, width), BF16),
        in_specs=[SMEM, VMEM, VMEM, VMEM, VMEM],
        out_specs=VMEM,
        compiler_params=room(4),
        name="second",
    )(offset, sums, again, wavefunction, preconditioner)
    pieces, _, _ = partial_pieces(over_terms(copies), left, right, False)
    sigma_second = pl.pallas_call(
        sum_kernel,
        out_shape=row_shape,
        in_specs=[VMEM],
        out_specs=VMEM,
        compiler_params=room(4),
        name="last",
    )(pieces)
    return (sigma_first, sigma_second)


def solution(mesh):
    torus = Mesh(mesh.devices.reshape(2, 4, 4, 2, 2), EVERY)
    placed = (
        P(SECTOR, None, None),
        P(OP, SECTOR, None, None),
        P(OP, SECTOR, None, None),
        P(OP, SECTOR),
        P(SECTOR, OP, None),
    )
    return jax.shard_map(
        on_device,
        mesh=torus,
        in_specs=placed,
        out_specs=(P(SECTOR, OP, None), P(SECTOR, OP, None)),
        check_vma=False,
    )
```

```python
import functools
import itertools
import random

import jax
import jax.numpy as jnp
from jax import lax
from jax.experimental import pallas as pl
from jax.experimental.pallas import tpu as pltpu
from jax.sharding import Mesh
from jax.sharding import PartitionSpec as P

SECTOR = ("sector_0", "sector_1")
OP = ("op_0", "op_1", "op_2")
EVERY = ("op_0", "op_1", "op_2", "sector_0", "sector_1")
CORE = "sector_1"
F32 = jnp.float32
BF16 = jnp.bfloat16
VMEM = pl.BlockSpec(memory_space=pltpu.VMEM)
SMEM = pl.BlockSpec(memory_space=pltpu.SMEM)
HBM = pl.BlockSpec(memory_space=pltpu.HBM)


def room(mebibytes):
    return pltpu.CompilerParams(vmem_limit_bytes=mebibytes * 2**20)


def place(op_0, op_1, op_2, half, core):
    return (((op_0 * 4 + op_1) * 4 + op_2) * 2 + half) * 2 + core


def mixed(members, seed):
    members = list(members)
    random.Random(seed).shuffle(members)
    return members


OP_ORDER = list(itertools.product(range(2), range(4), range(4)))
REST_ORDER = mixed(itertools.product(range(2), range(4), range(2)), 3)
REST_AT = [(low * 4 + at) * 2 + half for low, at, half in REST_ORDER]


def exchange(pieces, groups):
    return lax.all_to_all(
        pieces, EVERY, split_axis=0, concat_axis=0, axis_index_groups=groups, tiled=True
    )


def with_everyone(pieces):
    return exchange(pieces, [mixed(range(lax.axis_size(EVERY)), 0)])


def over_terms(pieces):
    sectors = itertools.product(range(2), range(2))
    return exchange(
        pieces, [[place(*op, half, core) for op in OP_ORDER] for half, core in sectors]
    )


def listed(targets, core, order, at):
    local_sectors, terms = targets.shape

    def scan(task, count):
        target = targets[lax.rem(task, local_sectors), task // local_sectors]
        order[count] = task
        return count + (lax.rem(target // local_sectors, 2) == core).astype(jnp.int32)

    return lax.fori_loop(0, local_sectors * terms, scan, at)


def slot_of(targets, task):
    local_sectors = targets.shape[0]
    target = targets[lax.rem(task, local_sectors), task // local_sectors]
    return target // (2 * local_sectors) * local_sectors + lax.rem(target, local_sectors)


def run_tasks(targets, order, begin, end, source, lefts, rights, totals, touched, arrive):
    local_sectors = targets.shape[0]

    def middle_of(task):
        vector = source(lax.rem(task, local_sectors))
        return jnp.dot(lefts[task], vector, preferred_element_type=F32).astype(BF16)

    def add(task, middle):
        slot = slot_of(targets, task)
        fresh = touched[slot] == 0
        touched[slot] = 1
        share = lax.dot_general(
            middle, rights[task], (((1,), (1,)), ((), ())), preferred_element_type=F32
        )
        totals[slot] = share + jnp.where(fresh, 0.0, totals[slot])

    def pair(index, carry):
        tasks = order[begin + 2 * index], order[begin + 2 * index + 1]
        for task in tasks:
            arrive(0, task)
        middles = [middle_of(task) for task in tasks]
        for task in tasks:
            arrive(1, task)
        for task, middle in zip(tasks, middles):
            add(task, middle)
        return carry

    lax.fori_loop(0, (end - begin) // 2, pair, 0)

    @pl.when(lax.rem(end - begin, 2) == 1)
    def _():
        task = order[end - 1]
        arrive(0, task)
        arrive(1, task)
        add(task, middle_of(task))


def clear(touched):
    for slot in range(touched.shape[0]):
        touched[slot] = 0


def fill(totals, touched):
    for slot in range(totals.shape[0]):

        @pl.when(touched[slot] == 0)
        def _(slot=slot):
            totals[slot] = jnp.zeros(totals.shape[1:], totals.dtype)


def early_kernel(first, targets, core, vector, left, right, out, kept, *refs):
    if first:
        lefts, rights, touched, order, totals, wave, known, sems, wave_sem, known_sem = refs
        whole = pltpu.make_async_copy(vector, wave, wave_sem)
        listing = pltpu.make_async_copy(targets, known, known_sem)
        listing.start()
        whole.start()
        listing.wait()
        targets = known
    else:
        lefts, rights = left, right
        touched, order, totals = refs
    tasks = lefts.shape[0]

    def copy(side, task):
        origin, buffer = ((left, lefts), (right, rights))[side]
        return pltpu.make_async_copy(origin.at[task], buffer.at[task], sems.at[side, task])

    def start(sides, index, carry):
        for side in sides:
            copy(side, order[index]).start()
        return carry

    def arrive(side, task):
        if first:
            copy(side, task).wait()

    def rest(index, carry):
        for side in (0, 1):
            arrive(side, order[index])
        return carry

    def source(sector):
        return wave[sector] if first else vector[:, sector].reshape(lefts.shape[1:])

    count = listed(targets, 1 - core[0], order, jnp.int32(0))
    listed(targets, core[0], order, count)
    if first:
        early = jnp.minimum(count, 2)
        lax.fori_loop(0, early, functools.partial(start, (0,)), 0)
        lax.fori_loop(0, early, functools.partial(start, (1,)), 0)
        lax.fori_loop(early, tasks, functools.partial(start, (0, 1)), 0)
        whole.wait()
    end = jnp.maximum(count, tasks // 2)
    clear(touched)
    run_tasks(targets, order, 0, count, source, lefts, rights, totals, touched, arrive)
    for slot in range(out.shape[0]):

        @pl.when(touched[slot] == 1)
        def _(slot=slot):
            out[slot] = totals[slot].astype(BF16)

    fill(out, touched)
    clear(touched)
    run_tasks(targets, order, count, end, source, lefts, rights, kept, touched, arrive)
    if first:
        lax.fori_loop(end, tasks, rest, 0)


def late_kernel(targets, core, vector, lefts, rights, begun, kept, touched, order):
    del begun
    tasks = lefts.shape[0]
    count = listed(targets, 1 - core[0], order, jnp.int32(0))
    listed(targets, core[0], order, count)
    end = jnp.maximum(count, tasks // 2)
    clear(touched)

    def mark(index, carry):
        touched[slot_of(targets, order[index])] = 1
        return carry

    def source(sector):
        whole = vector[sector] if vector.shape[1:] == lefts.shape[1:] else vector[:, sector]
        return whole.reshape(lefts.shape[1:])

    def arrive(side, task):
        del side, task

    lax.fori_loop(count, end, mark, 0)
    run_tasks(targets, order, end, tasks, source, lefts, rights, kept, touched, arrive)
    fill(kept, touched)


def apply_early(targets, core, vector, left, right, first):
    tasks, width, _ = left.shape
    slots = tasks // 2
    block = (slots, width, width)
    out = [jax.ShapeDtypeStruct(block, BF16), jax.ShapeDtypeStruct(block, F32)]
    scratch = [
        pltpu.SMEM((slots,), jnp.int32),
        pltpu.SMEM((tasks + 1,), jnp.int32),
        pltpu.VMEM(block, F32),
    ]
    if first:
        scratch += [
            pltpu.VMEM(vector.shape, BF16),
            pltpu.SMEM(targets.shape, jnp.int32),
            pltpu.SemaphoreType.DMA((2, tasks)),
            pltpu.SemaphoreType.DMA,
            pltpu.SemaphoreType.DMA,
        ]
        targets, vector, left, right = (
            pltpu.with_memory_space_constraint(value, pltpu.HBM)
            for value in (targets, vector, left, right)
        )
        out += [jax.ShapeDtypeStruct(left.shape, BF16)] * 2
    return pl.pallas_call(
        functools.partial(early_kernel, first),
        out_shape=out,
        in_specs=[HBM, SMEM, HBM, HBM, HBM] if first else [SMEM, SMEM, VMEM, VMEM, VMEM],
        out_specs=[VMEM] * len(out),
        scratch_shapes=scratch,
        compiler_params=room(8),
        cost_estimate=work(tasks, width),
        name="early_first" if first else "early",
    )(targets, core, vector, left, right)


def apply_late(targets, core, vector, left, right, begun):
    tasks, width, _ = left.shape
    return pl.pallas_call(
        late_kernel,
        out_shape=jax.ShapeDtypeStruct(begun.shape, F32),
        in_specs=[SMEM, SMEM] + [VMEM] * 4,
        out_specs=VMEM,
        scratch_shapes=[
            pltpu.SMEM((tasks // 2,), jnp.int32),
            pltpu.SMEM((tasks + 1,), jnp.int32),
        ],
        input_output_aliases={5: 0},
        compiler_params=room(8),
        cost_estimate=work(tasks, width),
        name="late",
    )(targets, core, vector, left, right, begun)


def work(tasks, width):
    return pl.CostEstimate(
        flops=2 * tasks * width**3, bytes_accessed=2 * tasks * width**2, transcendentals=0
    )


def along_ring(value, step):
    pairs = []
    for op_0, op_1, op_2, half in itertools.product(range(2), range(4), range(4), range(2)):
        first, second = (op_1 + step) % 4, (op_2 + step) % 4
        pairs.append((place(op_0, op_1, op_2, half, 0), place(op_0, first, op_2, half, 0)))
        pairs.append((place(op_0, op_1, op_2, half, 1), place(op_0, op_1, second, half, 1)))
    return lax.ppermute(value, EVERY, pairs)


def across_rings(pieces):
    rest = REST_ORDER
    groups = [[place(low, ring, at, half, 0) for low, at, half in rest] for ring in range(4)]
    groups += [[place(low, at, ring, half, 1) for low, at, half in rest] for ring in range(4)]
    return exchange(pieces, groups)


def pack_kernel(ring, core, kept, arrived, own, *sent):
    others, local_sectors, rows, _ = own.shape
    near, far = rows, 4 * rows
    ring_stride = jnp.where(core[0] == 0, far, near)
    at_stride = jnp.where(core[0] == 0, near, far)
    to = [lax.rem(ring[0] + step, 4) * ring_stride for step in range(4)]

    def one_place(place, carry):
        base = place // 4 * (16 * rows) + lax.rem(place, 4) * at_stride
        for step, half, sector in itertools.product(range(4), range(2), range(local_sectors)):
            here = pl.ds(pl.multiple_of(base + to[step], rows), rows)
            slot = half * local_sectors + sector
            total = kept[slot, here, :] + arrived[slot, here, :].astype(F32)
            if step == 0:
                own[2 * place + half, sector] = total
            else:
                sent[step - 1][2 * place + half, sector] = total.astype(BF16)
        return carry

    lax.fori_loop(0, others // 2, one_place, 0)


def pack(ring, core, kept, arrived, shape):
    return pl.pallas_call(
        pack_kernel,
        out_shape=[jax.ShapeDtypeStruct(shape, F32)] + [jax.ShapeDtypeStruct(shape, BF16)] * 3,
        in_specs=[SMEM, SMEM, VMEM, VMEM],
        out_specs=[VMEM] * 4,
        compiler_params=room(4),
        name="pack",
    )(ring, core, kept, arrived)


def meet_kernel(own, first, second, third, out):
    for to, index in enumerate(REST_AT):
        total = own[index] + first[index].astype(F32)
        total += second[index].astype(F32) + third[index].astype(F32)
        out[to] = total.astype(BF16)


def meet(own, arrived):
    return pl.pallas_call(
        meet_kernel,
        out_shape=jax.ShapeDtypeStruct(own.shape, BF16),
        in_specs=[VMEM] * 4,
        out_specs=VMEM,
        compiler_params=room(4),
        name="meet",
    )(own, *arrived)


def summed(pieces):
    shape = pieces.shape[1:]
    count = pieces.shape[0]

    def add(index, total):
        return total + pieces[index].astype(F32)

    return lax.fori_loop(0, count, add, jnp.zeros(shape, F32), unroll=8)


def lanes(value):
    local_sectors, rows, width = value.shape
    flat = jnp.sum(value.reshape(local_sectors * rows, width), axis=0, keepdims=True)
    return sum(flat[:, at : at + 128] for at in range(0, width, 128))


def first_kernel(offset, pieces, wave, precond, sigma, again, sums):
    rows = precond.shape[1]
    own = wave[:, pl.ds(pl.multiple_of(offset[0], rows), rows), :].astype(F32)
    total = summed(pieces)
    sigma[...] = total
    again[...] = total
    ratio, scaled = total / precond[...], own / precond[...]
    terms = (
        own * own,
        own * total,
        own * ratio,
        own * scaled,
        ratio * ratio,
        ratio * scaled,
        scaled * scaled,
    )
    one = jnp.concatenate([lanes(term) for term in terms] + [jnp.zeros((1, 128), F32)], axis=0)
    one = jnp.sum(one, axis=1, keepdims=True)
    row = lax.broadcasted_iota(jnp.int32, (8, 128), 0)
    lane = lax.broadcasted_iota(jnp.int32, (8, 128), 1)
    one = jnp.sum(jnp.where(row == lane, one, 0.0), axis=0, keepdims=True)
    sums[...] = jnp.broadcast_to(one[None], sums.shape)


def second_kernel(offset, sums, sigma, wave, precond, copies):
    rows = precond.shape[1]
    own = wave[:, pl.ds(pl.multiple_of(offset[0], rows), rows), :].astype(F32)
    whole = summed(sums)
    norm_sq, w_s, w_r, w_b, r_r, r_b, b_b = (whole[:, k : k + 1] for k in range(7))
    shift = w_s / norm_sq - 1.0
    projected = w_r - shift * w_b
    correction_sq = r_r - 2.0 * shift * r_b + shift * shift * b_b
    along = projected / norm_sq
    update_sq = jnp.maximum(correction_sq - projected * along, 0.0)
    scale = jnp.sqrt(norm_sq) * lax.rsqrt(update_sq + 1e-06)
    correction = (sigma[...] - shift[None] * own) / precond[...]
    new = ((correction - along[None] * own) * scale[None]).astype(BF16)
    copies[...] = jnp.broadcast_to(new[None], copies.shape)


def sum_kernel(pieces, sigma):
    sigma[...] = summed(pieces)


def on_device(wavefunction, left_blocks, right_blocks, target_sector, preconditioner):
    local_sectors, width, _ = wavefunction.shape
    rows = preconditioner.shape[1]
    owners = lax.axis_size(OP)
    offset = (lax.axis_index(OP) * rows).reshape(1)
    mine = lax.axis_index(CORE).reshape(1)
    ring = jnp.where(mine == 0, lax.axis_index("op_1"), lax.axis_index("op_2"))
    targets = target_sector.T
    left, right = (
        blocks.reshape(-1, width, width) for blocks in (left_blocks, right_blocks)
    )
    row_shape = jax.ShapeDtypeStruct((local_sectors, rows, width), F32)
    offset, mine, ring = lax.optimization_barrier((offset, mine, ring))

    def partial_pieces(vector, left, right, first):
        sent, begun, *blocks = apply_early(targets, mine, vector, left, right, first)
        left, right = blocks if first else (left, right)
        arrived = lax.ppermute(sent, CORE, [(0, 1), (1, 0)])
        kept = apply_late(targets, mine, vector, left, right, begun)
        shape = (owners // 2, local_sectors, rows, width)
        own, *sent = pack(ring, mine, kept, arrived, shape)
        arrived = [along_ring(sent[step - 1], step) for step in (2, 1, 3)]
        return across_rings(meet(own, arrived)), left, right

    pieces, left, right = partial_pieces(wavefunction, left, right, True)
    devices = lax.axis_size(EVERY)
    sigma_first, again, sums = pl.pallas_call(
        first_kernel,
        out_shape=(row_shape, row_shape, jax.ShapeDtypeStruct((devices, 1, 128), F32)),
        in_specs=[SMEM, VMEM, VMEM, VMEM],
        out_specs=(VMEM, VMEM, VMEM),
        compiler_params=room(4),
        name="first",
    )(offset, pieces, wavefunction, preconditioner)
    sums = with_everyone(sums)
    copies = pl.pallas_call(
        second_kernel,
        out_shape=jax.ShapeDtypeStruct((owners, local_sectors, rows, width), BF16),
        in_specs=[SMEM, VMEM, VMEM, VMEM, VMEM],
        out_specs=VMEM,
        compiler_params=room(4),
        name="second",
    )(offset, sums, again, wavefunction, preconditioner)
    pieces, _, _ = partial_pieces(over_terms(copies), left, right, False)
    sigma_second = pl.pallas_call(
        sum_kernel,
        out_shape=row_shape,
        in_specs=[VMEM],
        out_specs=VMEM,
        compiler_params=room(4),
        name="last",
    )(pieces)
    return (sigma_first, sigma_second)


def solution(mesh):
    torus = Mesh(mesh.devices.reshape(2, 4, 4, 2, 2), EVERY)
    placed = (
        P(SECTOR, None, None),
        P(OP, SECTOR, None, None),
        P(OP, SECTOR, None, None),
        P(OP, SECTOR),
        P(SECTOR, OP, None),
    )
    return jax.shard_map(
        on_device,
        mesh=torus,
        in_specs=placed,
        out_specs=(P(SECTOR, OP, None), P(SECTOR, OP, None)),
        check_vma=False,
    )
```
